512 devices in a mesh: row: 32 (over y, z_lo, core), col: 16 (over z_hi, x).
Axes of the slice: x: 4, y: 8, z: 8 (z_hi: 4, z_lo: 2; z = z_hi * 2 + z_lo), core: 2. Of those that a mesh axis runs over, the one named last changes fastest.
Arguments:
- residual: float32 [8192, 8192], P('row', 'col'), may hold values from -0.15625 to 0.15625
- direction: float32 [8192, 8192], P('row', 'col'), may hold values from -6 to 6
- ground_shift: float32 [1], replicated, may hold values from 1.6937256e-06 to 6.7749024e-06
- previous: float32 [1], replicated, may hold values from 3072 to 12288
Outputs:
- next_direction: float32 [8192, 8192], P('row', 'col')
- step_ratio: float32 [1], replicated
The draws below stay inside these ranges and needn't reach their ends.
All inputs are finite; a program needn't handle non-finite values.
Results may differ from the reference program's by a relative error of at most 0.00015.
Values sent between devices are 32-bit elements; how exact they have to be, the bound alone decides.
A program may use at most 64 MiB of HBM per device.

```python
import math
import jax
import jax.numpy as jnp
from jax import lax

Q0 = 256
NX = 8192
NY = 8192


def draw_residual(key, part):
    subkeys = jax.random.split(jax.random.fold_in(key, 17), 2)
    row_place = jnp.arange(NX, dtype=jnp.int32).astype(jnp.float32) / NX
    col_scale = jnp.exp(jax.random.uniform(subkeys[1], (NY,), jnp.float32, 0.0, jnp.log(10.0)))
    base_scale = 0.1 / Q0
    row_scale = jnp.exp(row_place * jnp.log(10.0))
    samples = jnp.clip(jax.random.normal(subkeys[0], (NX, NY), jnp.float32), -4.0, 4.0)
    return base_scale * row_scale[:, None] * col_scale[None, :] * samples


def shard_levels(key, dims, cuts, low, largest):
    level = 1.0
    for axis_at, blocks in cuts:
        steps = jax.random.uniform(jax.random.fold_in(jax.random.fold_in(key, 6), axis_at), (blocks,), jnp.float32, low / len(cuts), largest / len(cuts))
        level = level * jnp.repeat(jnp.exp(steps), dims[axis_at] // blocks).reshape((-1,) + (1,) * (len(dims) - 1 - axis_at))
    return level


def gaussian(rng, dims, scale, reach, pieces=(), held_as=jnp.bfloat16):
    result = jax.random.normal(rng, dims, jnp.float32) * scale
    if len(pieces) > 0:
        result = shard_levels(rng, dims, pieces, -0.22, 0.18) * result
    return jnp.clip(result, min=-reach, max=reach).astype(held_as)


def setup_inputs(seed: int = 0) -> dict:
    streams_of = jax.random.split(jax.random.key(seed), 5)
    residual = draw_residual(jax.random.fold_in(streams_of[4], 71), 0)
    direction = gaussian(streams_of[1], (NX, NY), 1.0, 6.0, ((0, 32), (1, 16)), jnp.float32)
    ground_shift = jnp.clip(jnp.exp(jax.random.uniform(streams_of[2], (1,), jnp.float32, math.log(1.6937256077653728e-06), math.log(6.774902431061491e-06))), 1.6937256077653728e-06, 6.774902431061491e-06)
    previous = jnp.clip(jnp.exp(jax.random.uniform(streams_of[3], (1,), jnp.float32, math.log(3072.0), math.log(12288.0))), 3072.0, 12288.0)
    return dict(residual=residual, direction=direction, ground_shift=ground_shift, previous=previous)


PRECISE = lax.Precision.HIGHEST

def cosine_matrix(length):
    wavenum = jnp.arange(length, dtype=jnp.int32)[:, None]
    position = jnp.arange(length, dtype=jnp.int32)[None, :]
    phases = wavenum * (2 * position + 1) % (4 * length)
    angles = jnp.pi * phases.astype(jnp.float32) / (2 * length)
    scaling = jnp.where(wavenum == 0, jnp.sqrt(1.0 / length), jnp.sqrt(2.0 / length)).astype(jnp.float32)
    return scaling * jnp.cos(angles)

def reference(residual, direction, ground_shift, previous):
    rows_table = cosine_matrix(NX)
    cols_table = cosine_matrix(NY)
    spectrum = jnp.dot(jnp.dot(rows_table, residual, precision=PRECISE), cols_table.T, precision=PRECISE)
    row_waves = jnp.arange(NX, dtype=jnp.int32).astype(jnp.float32)
    col_waves = jnp.arange(NY, dtype=jnp.int32).astype(jnp.float32)
    row_sine = jnp.sin(jnp.pi * row_waves / (2 * NX))
    col_sine = jnp.sin(jnp.pi * col_waves / (2 * NY))
    eigenvalue = 4.0 * (row_sine * row_sine)[:, None] + 4.0 * (col_sine * col_sine)[None, :]
    weight = 1.0 / (eigenvalue + ground_shift[0])
    scaled = weight * spectrum
    precond = jnp.dot(jnp.dot(rows_table.T, scaled, precision=PRECISE), cols_table, precision=PRECISE)
    inner_total = jnp.sum(residual * precond)
    step_ratio = inner_total / previous[0]
    return (precond + step_ratio * direction, jnp.reshape(step_ratio, (1,)))
```

```python
import math
import jax
import jax.numpy as jnp
import numpy as np
from jax import lax
from jax.sharding import PartitionSpec as P

HI = lax.Precision.HIGHEST


def mm(a, b, ca=1, cb=0):
    return lax.dot_general(
        a, b, (((ca,), (cb,)), ((), ())), precision=HI, preferred_element_type=jnp.float32
    )


def dct_table(n):
    k = np.arange(n)[:, None]
    p = np.arange(n)[None, :]
    table = np.sqrt(2.0 / n) * np.cos(np.pi * (k * (2 * p + 1) % (4 * n)) / (2 * n))
    table[0] = np.sqrt(1.0 / n)
    return table


def edge_sines(blocks):
    e = np.arange(1, blocks)
    q = np.zeros((blocks, blocks))
    q[: blocks - 1, : blocks - 1] = np.sqrt(2.0 / blocks) * np.sin(
        np.pi * (np.outer(e, e) % (2 * blocks)) / blocks
    )
    return q


def make_tables(n, w, R, C):
    assert w == 2 * n
    M = n // 2
    f = {}
    cn, cw = dct_table(n), dct_table(w)
    phi, sgn = cn[:, 0], np.where(np.arange(n) % 2 == 0, 1.0, -1.0)
    phj, sgj = cw[:, 0], np.where(np.arange(w) % 2 == 0, 1.0, -1.0)
    lam_i = 4 * np.sin(np.pi * np.arange(n) / (2 * n)) ** 2
    lam_j = 4 * np.sin(np.pi * np.arange(w) / (2 * w)) ** 2
    f["cn"], f["cw"] = cn, cw
    f["lam"] = lam_i[:, None] + lam_j[None, :]
    f["lamj"] = np.tile(lam_j[None, :], (8, 1))
    p1 = np.zeros((8, n))
    p1[0], p1[1] = phi, sgn * phi
    p2 = np.zeros((8, w))
    p2[0], p2[1] = phj, sgj * phj
    f["p1"], f["p2"] = p1, p2
    f["ph8"] = np.concatenate([np.tile(p2[0:1], (4, 1)), np.tile(p2[1:2], (4, 1))])
    even = (sgn > 0) * phi
    odd = (sgn < 0) * phi
    f["m8"] = np.stack([even, even, odd, odd, even, even, odd, odd])

    t = np.arange(R)[:, None]
    d = np.arange(R)[None, :]
    ang = np.pi * (t * d % (2 * R)) / R
    mix_c, mix_s = np.cos(ang), np.sin(ang)
    mix_s[0] = np.where(np.arange(R) % 2 == 0, 1.0, -1.0)
    q_r, q_c = edge_sines(R), edge_sines(C)
    last_r = q_r.T.copy()
    first_r = np.zeros((R, R))
    first_r[:, 1:] = -q_r.T[:, :-1]
    last_c = q_c.T.copy()
    first_c = np.zeros((C, C))
    first_c[:, 1:] = -q_c.T[:, :-1]

    qe = np.zeros((2, R, R, 8))
    for h in range(2):
        qe[h, :, :, h] = first_r
        qe[h, :, :, 2 + h] = last_r
    f["qe"] = qe.reshape(2 * R, 8 * R)
    qc = np.zeros((2 * C + 8, C, 8))
    for a in range(2):
        qc[a * C : (a + 1) * C, :, 2 * a] = first_c
        qc[a * C : (a + 1) * C, :, 2 * a + 1] = last_c
    qc[2 * C, :, 4] = 1.0
    f["qc"] = qc.reshape(2 * C + 8, 8 * C)

    nxt = lambda m: np.concatenate([m[:, 1:], np.zeros((R, 1))], axis=1)
    x3 = np.zeros((2, 2, R, R, 8))
    for side in range(2):
        for part, mix in ((0, mix_c), (2, mix_s)):
            x3[0, side, :, :, part + side] = q_r.T @ (mix - nxt(mix)).T
            x3[1, side, :, :, part + side] = -q_r.T @ (mix + nxt(mix)).T
    f["x3"] = x3.reshape(4 * R, 8 * R)

    p = np.arange(n)[:, None]
    m = np.arange(M)[None, :]
    a_ang = np.pi * (m * (2 * p + 1) % (2 * n)) / n
    tab = np.concatenate([np.cos(a_ang), np.sin(a_ang)], axis=1)
    f["tab"] = tab
    f["tabt"] = np.concatenate([np.cos(a_ang).T, np.sin(a_ang).T], axis=1)

    lanes = max(8 * R, n, 2 * M)
    dev = np.zeros((R, 48, lanes))
    pos = 2 * np.arange(n) + 1
    N = n * R
    shift_r = np.zeros((R, R))
    shift_r[1:] = q_r[:-1]
    for r in range(R):
        nz = float(r > 0)
        for part, mix in ((0, mix_c), (1, mix_s)):
            for side in range(2):
                row = np.zeros((R, 8))
                row[:, 4 + side] = mix[r]
                dev[r, 2 * part + side, : 8 * R] = row.reshape(-1)
        row = np.zeros((R, 8))
        row[:, 6] = 1.0
        dev[r, 4, : 8 * R] = row.reshape(-1)
        for rep in range(2):
            for part, mix in ((0, mix_c), (1, mix_s)):
                top = mix[r] @ shift_r
                bot = -(mix[r] @ q_r)
                dev[r, 8 + 4 * rep + part, :R] = top + bot
                dev[r, 8 + 4 * rep + 2 + part, :R] = top - bot
        dev[r, 16, :R] = shift_r[r]
        dev[r, 17, :R] = -q_r[r]
        for side in range(2):
            row = np.zeros((R, 8))
            row[:, side] = mix_c[:, r]
            row[:, 2 + side] = mix_s[:, r]
            dev[r, 24 + side, : 8 * R] = row.reshape(-1)
        row = np.zeros((R, 8))
        row[:, 4] = 1.0
        dev[r, 26, : 8 * R] = row.reshape(-1)
        tau = (r, 2 * R - r if r > 0 else R)
        ca, sa = [], []
        for x in tau:
            b = np.pi * (x * pos % (4 * N)) / (2 * N)
            ca.append(np.cos(b))
            sa.append(np.sin(b))
        rot = [ca[0], -nz * sa[0], sa[0], nz * ca[0]]
        if r > 0:
            rot += [ca[1], sa[1], sa[1], -ca[1]]
        else:
            rot += [0 * pos, ca[1], 0 * pos, sa[1]]
        for i, v in enumerate(rot):
            dev[r, 32 + i, :n] = v
        k = np.concatenate([2 * R * np.arange(M) + x for x in tau])
        dev[r, 40, : 2 * M] = 4 * np.sin(np.pi * k / (2 * N)) ** 2
        dev[r, 41, : 2 * M] = np.where(k == 0, 1.0 / N, 2.0 / N)
    f["dev"] = dev
    shift_c = np.zeros((C, C))
    shift_c[1:] = q_c[:-1]
    devc = np.zeros((C, 8, max(128, C)))
    for c in range(C):
        devc[c, 0, :C] = shift_c[c]
        devc[c, 1, :C] = -q_c[c]
    f["devc"] = devc
    f["s2r"] = np.tile(np.sin(np.pi * np.arange(1, R + 1) / (2 * R))[:, None] ** 2, (1, 128))
    f["s2c"] = np.tile(np.sin(np.pi * np.arange(1, C + 1) / (2 * C))[:, None] ** 2, (1, 128))
    return {key: v.astype(np.float32) for key, v in f.items()}


def chain(mu, n):
    s = 0.5 * jnp.sqrt(mu)
    ch = jnp.sqrt(1.0 + s * s)
    x = s + s * s / (1.0 + ch)
    z = x / (2.0 + x)
    z2 = z * z
    acc = jnp.full_like(z, 1.0 / 19.0)
    for k in (17, 15, 13, 11, 9, 7, 5, 3, 1):
        acc = acc * z2 + 1.0 / k
    theta = 4.0 * z * acc
    decay = jnp.exp(-n * theta)
    shorter = jnp.exp(-(n - 1) * theta)
    diff = (ch - s) * (1.0 - shorter) / (2.0 * s * (1.0 + decay))
    far = ch * decay / (s * (1.0 - decay * decay))
    return 1.0 + 2.0 * diff, 4.0 * far


def phase_a(r, g, f):
    n = f["cn"].shape[0]
    spec = mm(f["cn"], mm(r, f["cw"], 1, 1))
    weight = 1.0 / (f["lam"] + g)
    sol = weight * spec
    energy = jnp.sum(spec * sol)
    zfl = mm(f["p1"], sol)
    zb = mm(f["p2"], sol, 1, 1)
    lane = jnp.full((1, n), energy, jnp.float32)
    out = jnp.concatenate(
        [zfl[0:1, :n], zfl[0:1, n:], zfl[1:2, :n], zfl[1:2, n:], zb[0:2], lane, zb[3:4]], axis=0
    )
    return spec, weight, out


def phase_b(buf, weight, g, f, dev):
    R8, n = buf.shape
    R = R8 // 8
    M = n // 2
    y2 = mm(f["qe"], buf)
    yl = jnp.concatenate([y2[:R], y2[R:]], axis=1)
    base, far = chain(f["lamj"][0:1] + g, n)
    inv = 1.0 / (base + far * f["s2r"][:, 0:1])
    tl = yl * inv
    energy_r = jnp.sum(yl * tl)
    mixed = mm(dev[0:8, :R8], buf)
    q8 = mm(dev[8:16, :R], tl) * f["ph8"]
    v8 = mm(q8, weight, 1, 1) * f["m8"]
    z4 = jnp.concatenate(
        [
            mixed[0:1] + v8[0:1] + v8[2:3],
            mixed[1:2] + v8[4:5] + v8[6:7],
            mixed[2:3] + v8[1:2] + v8[3:4],
            mixed[3:4] + v8[5:6] + v8[7:8],
        ],
        axis=0,
    )
    zp = mm(z4, f["cn"])
    re, im = zp[0:2], zp[2:4]
    rot = dev[32:40, :n]
    a1 = re * rot[0:1] + im * rot[1:2]
    b1 = re * rot[2:3] + im * rot[3:4]
    a2 = re * rot[4:5] + im * rot[5:6]
    b2 = re * rot[6:7] + im * rot[7:8]
    yy = mm(jnp.concatenate([a1, a2, b1, b2], axis=0), f["tab"])
    y4 = yy[0:4, :M] - yy[4:8, M:]
    strip = mixed[4:5, :M] - energy_r
    out = jnp.concatenate([y4, strip, jnp.zeros((3, M), jnp.float32)], axis=0)
    return yl, inv, out


def phase_c(buf, g, f, dev, devc):
    C8, M = buf.shape
    C = C8 // 8
    n = 2 * M
    y2 = mm(f["qc"], buf)
    y = jnp.concatenate([y2[:C], y2[C : 2 * C]], axis=1)
    total = y2[2 * C : 2 * C + 1, 0:1]
    base, far = chain(dev[40:41, : 2 * M] + g, 2 * n)
    tl = y / (base + far * f["s2c"][:, 0:1]) * dev[41:42, : 2 * M]
    energy_c = jnp.sum(y * tl)
    q2 = mm(devc[:, :C], tl)
    uv = mm(jnp.concatenate([q2[0:2, :M], q2[0:2, M:]], axis=0), f["tabt"])
    u1, u2 = uv[0:2, :n], uv[2:4, :n]
    v1, v2 = uv[0:2, n:], uv[2:4, n:]
    rot = dev[32:40, :n]
    re = u1 * rot[0:1] - v1 * rot[2:3] + u2 * rot[4:5] - v2 * rot[6:7]
    im = u1 * rot[1:2] - v1 * rot[3:4] + u2 * rot[5:6] - v2 * rot[7:8]
    lane = jnp.full((1, n), energy_c, jnp.float32)
    out = jnp.concatenate([re, im, lane, jnp.zeros((3, n), jnp.float32)], axis=0)
    return total, out


def phase_d(buf, spec, weight, yl, inv, total, direction, previous, f, dev):
    R8, n = buf.shape
    R = R8 // 8
    xx = mm(mm(f["x3"], buf), f["cn"], 1, 1)
    src = xx[: 2 * R] * f["m8"][0:1] + xx[2 * R :] * f["m8"][2:3]
    moved = mm(src, weight)
    y_all = yl + moved[:R] * f["p2"][0:1] + moved[R:] * f["p2"][1:2]
    row_flux = mm(dev[16:24, :R], y_all * inv)
    own = mm(dev[24:32, :R8], buf)
    inner = total - own[2:3, 0:1]
    sides = mm(own, f["cn"], 1, 1)
    left = jnp.concatenate([f["p1"], sides], axis=0)
    right = jnp.concatenate([row_flux, f["p2"]], axis=0)
    sol = weight * (spec + mm(left, right, 0, 0))
    precond = mm(f["cn"], mm(sol, f["cw"]), 0, 0)
    step_ratio = inner / previous
    return precond + step_ratio * direction, step_ratio


def solution(mesh):
    R, C = mesh.shape["row"], mesh.shape["col"]

    def body(residual, direction, ground_shift, previous):
        n, w = residual.shape
        f = {key: jnp.asarray(v) for key, v in make_tables(n, w, R, C).items()}
        g = ground_shift.reshape(1, 1)
        dev = f["dev"][lax.axis_index("row")]
        devc = f["devc"][lax.axis_index("col")]
        spec, weight, out = phase_a(residual, g, f)
        buf = lax.all_gather(out, "row", axis=0, tiled=True)
        yl, inv, out = phase_b(buf, weight, g, f, dev)
        buf = lax.all_gather(out, "col", axis=0, tiled=True)
        total, out = phase_c(buf, g, f, dev, devc)
        buf = lax.all_gather(out, "row", axis=0, tiled=True)
        res, ratio = phase_d(
            buf, spec, weight, yl, inv, total, direction, previous.reshape(1, 1), f, dev
        )
        return res, ratio.reshape(1)

    return jax.shard_map(
        body,
        mesh=mesh,
        in_specs=(P("row", "col"), P("row", "col"), P(), P()),
        out_specs=(P("row", "col"), P()),
        check_vma=False,
    )
```

```python
import functools
import jax
import jax.numpy as jnp
import numpy as np
from jax import lax
from jax.experimental import pallas as pl
from jax.experimental.pallas import tpu as pltpu
from jax.sharding import PartitionSpec as P

HI = lax.Precision.HIGHEST


def mm(a, b, ca=1, cb=0):
    return lax.dot_general(
        a[...], b[...], (((ca,), (cb,)), ((), ())), precision=HI, preferred_element_type=jnp.float32
    )


def dct_table(n):
    k = np.arange(n)[:, None]
    p = np.arange(n)[None, :]
    table = np.sqrt(2.0 / n) * np.cos(np.pi * (k * (2 * p + 1) % (4 * n)) / (2 * n))
    table[0] = np.sqrt(1.0 / n)
    return table


def edge_sines(blocks):
    e = np.arange(1, blocks)
    q = np.zeros((blocks, blocks))
    q[: blocks - 1, : blocks - 1] = np.sqrt(2.0 / blocks) * np.sin(
        np.pi * (np.outer(e, e) % (2 * blocks)) / blocks
    )
    return q


def make_tables(n, w, R, C):
    assert w == 2 * n
    M = n // 2
    f = {}
    cn, cw = dct_table(n), dct_table(w)
    phi, sgn = cn[:, 0], np.where(np.arange(n) % 2 == 0, 1.0, -1.0)
    phj, sgj = cw[:, 0], np.where(np.arange(w) % 2 == 0, 1.0, -1.0)
    lam_i = 4 * np.sin(np.pi * np.arange(n) / (2 * n)) ** 2
    lam_j = 4 * np.sin(np.pi * np.arange(w) / (2 * w)) ** 2
    f["cn"], f["cw"] = cn, cw
    f["lami"] = np.tile(lam_i[:, None], (1, 128))
    f["cnt"] = cn.T
    f["lamj"] = np.tile(lam_j[None, :], (8, 1))
    p1 = np.zeros((8, n))
    p1[0], p1[1] = phi, sgn * phi
    p2 = np.zeros((8, w))
    p2[0], p2[1] = phj, sgj * phj
    f["p1"], f["p2"] = p1, p2
    f["ph8"] = np.concatenate([np.tile(p2[0:1], (4, 1)), np.tile(p2[1:2], (4, 1))])
    even = (sgn > 0) * phi
    odd = (sgn < 0) * phi
    f["m8"] = np.stack([even, even, odd, odd, even, even, odd, odd])

    t = np.arange(R)[:, None]
    d = np.arange(R)[None, :]
    ang = np.pi * (t * d % (2 * R)) / R
    mix_c, mix_s = np.cos(ang), np.sin(ang)
    mix_s[0] = np.where(np.arange(R) % 2 == 0, 1.0, -1.0)
    q_r, q_c = edge_sines(R), edge_sines(C)
    last_r = q_r.T.copy()
    first_r = np.zeros((R, R))
    first_r[:, 1:] = -q_r.T[:, :-1]
    last_c = q_c.T.copy()
    first_c = np.zeros((C, C))
    first_c[:, 1:] = -q_c.T[:, :-1]

    qe = np.zeros((2, R, R, 8))
    for h in range(2):
        qe[h, :, :, h] = first_r
        qe[h, :, :, 2 + h] = last_r
    f["qe"] = qe.reshape(2 * R, 8 * R)
    qc = np.zeros((2 * C + 8, C, 8))
    for a in range(2):
        qc[a * C : (a + 1) * C, :, 2 * a] = first_c
        qc[a * C : (a + 1) * C, :, 2 * a + 1] = last_c
    qc[2 * C, :, 4] = 1.0
    f["qc"] = qc.reshape(2 * C + 8, 8 * C)

    nxt = lambda m: np.concatenate([m[:, 1:], np.zeros((R, 1))], axis=1)
    x3 = np.zeros((2, 2, R, R, 8))
    for side in range(2):
        for part, mix in ((0, mix_c), (2, mix_s)):
            x3[0, side, :, :, part + side] = q_r.T @ (mix - nxt(mix)).T
            x3[1, side, :, :, part + side] = -q_r.T @ (mix + nxt(mix)).T
    f["x3"] = x3.reshape(4 * R, 8 * R)

    p = np.arange(n)[:, None]
    m = np.arange(M)[None, :]
    a_ang = np.pi * (m * (2 * p + 1) % (2 * n)) / n
    tab = np.concatenate([np.cos(a_ang), np.sin(a_ang)], axis=1)
    f["tab"] = tab
    f["tabt"] = np.concatenate([np.cos(a_ang).T, np.sin(a_ang).T], axis=1)

    lanes = max(8 * R, n, 2 * M, 256)
    dev = np.zeros((R, 32, lanes))
    pos = 2 * np.arange(n) + 1
    N = n * R
    shift_r = np.zeros((R, R))
    shift_r[1:] = q_r[:-1]
    for r in range(R):
        nz = float(r > 0)
        for part, mix in ((0, mix_c), (1, mix_s)):
            for side in range(2):
                row = np.zeros((R, 8))
                row[:, 4 + side] = mix[r]
                dev[r, 2 * part + side, : 8 * R] = row.reshape(-1)
        row = np.zeros((R, 8))
        row[:, 6] = 1.0
        dev[r, 4, : 8 * R] = row.reshape(-1)
        for rep in range(2):
            for part, mix in ((0, mix_c), (1, mix_s)):
                top = mix[r] @ shift_r
                bot = -(mix[r] @ q_r)
                dev[r, 8 + 4 * rep + part, :R] = top + bot
                dev[r, 8 + 4 * rep + 2 + part, :R] = top - bot
        dev[r, 8, 128 : 128 + R] = shift_r[r]
        dev[r, 9, 128 : 128 + R] = -q_r[r]
        for side in range(2):
            row = np.zeros((R, 8))
            row[:, side] = mix_c[:, r]
            row[:, 2 + side] = mix_s[:, r]
            dev[r, 16 + side, : 8 * R] = row.reshape(-1)
        row = np.zeros((R, 8))
        row[:, 4] = 1.0
        dev[r, 18, : 8 * R] = row.reshape(-1)
        tau = (r, 2 * R - r if r > 0 else R)
        ca, sa = [], []
        for x in tau:
            b = np.pi * (x * pos % (4 * N)) / (2 * N)
            ca.append(np.cos(b))
            sa.append(np.sin(b))
        rot = [ca[0], -nz * sa[0], sa[0], nz * ca[0]]
        if r > 0:
            rot += [ca[1], sa[1], sa[1], -ca[1]]
        else:
            rot += [0 * pos, ca[1], 0 * pos, sa[1]]
        for i, v in enumerate(rot):
            dev[r, 24 + i, :n] = v
        k = np.concatenate([2 * R * np.arange(M) + x for x in tau])
        dev[r, 5, : 2 * M] = 4 * np.sin(np.pi * k / (2 * N)) ** 2
        dev[r, 6, : 2 * M] = np.where(k == 0, 1.0 / N, 2.0 / N)
    f["dev"] = dev
    shift_c = np.zeros((C, C))
    shift_c[1:] = q_c[:-1]
    devc = np.zeros((C, 8, max(128, C)))
    for c in range(C):
        devc[c, 0, :C] = shift_c[c]
        devc[c, 1, :C] = -q_c[c]
    f["devc"] = devc
    f["s2r"] = np.tile(np.sin(np.pi * np.arange(1, R + 1) / (2 * R))[:, None] ** 2, (1, 128))
    f["s2c"] = np.tile(np.sin(np.pi * np.arange(1, C + 1) / (2 * C))[:, None] ** 2, (1, 128))
    return {key: v.astype(np.float32) for key, v in f.items()}


def chain(mu, n):
    s = 0.5 * jnp.sqrt(mu)
    ch = jnp.sqrt(1.0 + s * s)
    x = s + s * s / (1.0 + ch)
    z = x / (2.0 + x)
    z2 = z * z
    acc = jnp.full_like(z, 1.0 / 19.0)
    for k in (17, 15, 13, 11, 9, 7, 5, 3, 1):
        acc = acc * z2 + 1.0 / k
    theta = 4.0 * z * acc
    decay = jnp.exp(-n * theta)
    shorter = jnp.exp(-(n - 1) * theta)
    diff = (ch - s) * (1.0 - shorter) / (2.0 * s * (1.0 + decay))
    far = ch * decay / (s * (1.0 - decay * decay))
    return 1.0 + 2.0 * diff, 4.0 * far


def phase_a(r, g, f):
    n = f["cn"].shape[0]
    spec = mm(f["cn"], mm(r, f["cw"], 1, 1))
    weight = 1.0 / (f["lami"][...][:, 0:1] + f["lamj"][0:1] + g)
    sol = weight * spec
    energy = jnp.sum(spec * sol, axis=0, keepdims=True)
    zfl = mm(f["p1"], sol)
    zb = mm(f["p2"], sol, 1, 1)
    lane = energy[:, :n] + energy[:, n:]
    out = jnp.concatenate(
        [zfl[0:1, :n], zfl[0:1, n:], zfl[1:2, :n], zfl[1:2, n:], zb[0:2], lane, zb[3:4]], axis=0
    )
    return spec, weight, out


def phase_b(buf, weight, g, f, dev):
    R8, n = buf.shape
    R = R8 // 8
    M = n // 2
    y2 = mm(f["qe"], buf)
    yl = jnp.concatenate([y2[:R], y2[R:]], axis=1)
    base, far = chain(f["lamj"][0:1] + g, n)
    inv = 1.0 / (base + far * f["s2r"][...][:, 0:1])
    tl = yl * inv
    energy_r = jnp.sum(yl * tl, axis=0, keepdims=True)
    mixed = mm(dev[0:8, :R8], buf)
    q8 = mm(dev[8:16, :R], tl) * f["ph8"]
    v8 = mm(q8, weight, 1, 1) * f["m8"]
    z4 = jnp.concatenate(
        [
            mixed[0:1] + v8[0:1] + v8[2:3],
            mixed[1:2] + v8[4:5] + v8[6:7],
            mixed[2:3] + v8[1:2] + v8[3:4],
            mixed[3:4] + v8[5:6] + v8[7:8],
        ],
        axis=0,
    )
    zp = mm(z4, f["cn"])
    re, im = zp[0:2], zp[2:4]
    rot = dev[24:32, :n]
    a1 = re * rot[0:1] + im * rot[1:2]
    b1 = re * rot[2:3] + im * rot[3:4]
    a2 = re * rot[4:5] + im * rot[5:6]
    b2 = re * rot[6:7] + im * rot[7:8]
    yy = mm(jnp.concatenate([a1, a2, b1, b2], axis=0), f["tab"])
    y4 = yy[0:4, :M] - yy[4:8, M:]
    strip = mixed[4:5] - (energy_r[:, :n] + energy_r[:, n:])
    strip = strip[:, :M] + strip[:, M:]
    out = jnp.concatenate([y4, strip, jnp.zeros((3, M), jnp.float32)], axis=0)
    return yl, inv, out


def phase_c(buf, g, f, dev, devc):
    C8, M = buf.shape
    C = C8 // 8
    n = 2 * M
    y2 = mm(f["qc"], buf)
    y = jnp.concatenate([y2[:C], y2[C : 2 * C]], axis=1)
    total = y2[2 * C : 2 * C + 1]
    base, far = chain(dev[5:6, : 2 * M] + g, 2 * n)
    tl = y / (base + far * f["s2c"][...][:, 0:1]) * dev[6:7, : 2 * M]
    energy_c = jnp.sum(y * tl, axis=0, keepdims=True)
    q2 = mm(devc[:, :C], tl)
    uv = mm(jnp.concatenate([q2[0:2, :M], q2[0:2, M:]], axis=0), f["tabt"])
    u1, u2 = uv[0:2, :n], uv[2:4, :n]
    v1, v2 = uv[0:2, n:], uv[2:4, n:]
    rot = dev[24:32, :n]
    re = u1 * rot[0:1] - v1 * rot[2:3] + u2 * rot[4:5] - v2 * rot[6:7]
    im = u1 * rot[1:2] - v1 * rot[3:4] + u2 * rot[5:6] - v2 * rot[7:8]
    out = jnp.concatenate([re, im, energy_c, jnp.zeros((3, n), jnp.float32)], axis=0)
    return total, out


def phase_d(buf, spec, weight, yl, inv, total, f, dev):
    R8, n = buf.shape
    R = R8 // 8
    xx = mm(mm(f["x3"], buf), f["cn"], 1, 1)
    src = xx[: 2 * R] * f["m8"][0:1] + xx[2 * R :] * f["m8"][2:3]
    moved = mm(src, weight)
    y_all = yl + moved[:R] * f["p2"][0:1] + moved[R:] * f["p2"][1:2]
    row_flux = mm(dev[8:16, 128 : 128 + R], y_all * inv)
    own = mm(dev[16:24, :R8], buf)
    inner = jnp.sum(total, axis=1, keepdims=True) - jnp.sum(own[2:3], axis=1, keepdims=True)
    sides = mm(own, f["cn"], 1, 1)
    left = jnp.concatenate([f["p1"], sides], axis=0)
    right = jnp.concatenate([row_flux, f["p2"]], axis=0)
    sol = weight * (spec + mm(left.T, right))
    return mm(f["cnt"], mm(sol, f["cw"])), inner


MESH_ID = pl.DeviceIdType.MESH


def kernel(names, R, C, *refs):
    count = len(names)
    shift_ref, residual_ref = refs[0], refs[1]
    table_hbm = refs[2 : 2 + count]
    precond_ref, inner_ref = refs[2 + count : 4 + count]
    r_v = refs[4 + count]
    table_v = refs[5 + count : 5 + 2 * count]
    out1, out2, out3, buf1, buf2, buf3 = refs[5 + 2 * count : 11 + 2 * count]
    load_sem, s1, v1, s2, v2, s3, v3 = refs[11 + 2 * count :]
    row, col = lax.axis_index("row"), lax.axis_index("col")

    barrier = pltpu.get_barrier_semaphore()

    @pl.loop(1, R)
    def _(i):
        peer = lax.rem(row + i, R)
        pl.semaphore_signal(barrier, inc=1, device_id=(peer, col), device_id_type=MESH_ID)

    @pl.loop(1, C)
    def _(i):
        peer = lax.rem(col + i, C)
        pl.semaphore_signal(barrier, inc=1, device_id=(row, peer), device_id_type=MESH_ID)

    loads = {"residual": pltpu.make_async_copy(residual_ref, r_v, load_sem.at[count])}
    for i, name in enumerate(names):
        src = table_hbm[i]
        if name == "dev":
            src = src.at[row]
        elif name == "devc":
            src = src.at[col]
        loads[name] = pltpu.make_async_copy(src, table_v[i], load_sem.at[i])
    loads["residual"].start()
    for name in names:
        loads[name].start()
    loads["residual"].wait()
    for name in names:
        loads[name].wait()
    f = {name: table_v[i] for i, name in enumerate(names)}
    f = {name: ref[...] if ref.shape[0] <= 32 else ref for name, ref in f.items()}
    dev, devc = f["dev"], f["devc"]
    g = shift_ref[0, 0]

    def share(out_ref, buf, send, recv, axis, size, me):
        def dest(peer):
            return (peer, col) if axis == 0 else (row, peer)

        def copy(peer, slot):
            return pltpu.make_async_remote_copy(
                src_ref=out_ref,
                dst_ref=buf.at[pl.ds(pl.multiple_of(slot * 8, 8), 8), :],
                send_sem=send.at[peer],
                recv_sem=recv.at[slot],
                device_id=dest(peer),
                device_id_type=MESH_ID,
            )

        @pl.loop(1, size)
        def _(i):
            copy(lax.rem(me + i, size), me).start()

        buf[pl.ds(pl.multiple_of(me * 8, 8), 8), :] = out_ref[...]

        @pl.loop(1, size)
        def _(i):
            peer = lax.rem(me + i, size)
            copy(peer, peer).wait_recv()

        def drain():
            @pl.loop(1, size)
            def _(i):
                copy(lax.rem(me + i, size), me).wait_send()

        return drain

    spec, weight, out = phase_a(r_v[...], g, f)
    out1[...] = out
    pl.semaphore_wait(barrier, R + C - 2)
    drain1 = share(out1, buf1, s1, v1, 0, R, row)
    yl, inv, out = phase_b(buf1[...], weight, g, f, dev)
    out2[...] = out
    drain2 = share(out2, buf2, s2, v2, 1, C, col)
    total, out = phase_c(buf2[...], g, f, dev, devc)
    out3[...] = out
    drain3 = share(out3, buf3, s3, v3, 0, R, row)
    precond, inner = phase_d(buf3[...], spec, weight, yl, inv, total, f, dev)
    precond_ref[...] = precond
    inner_ref[...] = jnp.broadcast_to(inner, inner_ref.shape)
    drain1()
    drain2()
    drain3()


def solution(mesh):
    R, C = mesh.shape["row"], mesh.shape["col"]

    def body(residual, direction, ground_shift, previous):
        n, w = residual.shape
        tables = make_tables(n, w, R, C)
        names = tuple(tables)
        shapes = [v.shape[1:] if k in ("dev", "devc") else v.shape for k, v in tables.items()]
        any_spec = pl.BlockSpec(memory_space=pltpu.HBM)
        vmem = pl.BlockSpec(memory_space=pltpu.VMEM)
        f32 = jnp.float32
        dma = pltpu.SemaphoreType.DMA
        precond, inner = pl.pallas_call(
            functools.partial(kernel, names, R, C),
            out_shape=(jax.ShapeDtypeStruct((n, w), f32), jax.ShapeDtypeStruct((8, 128), f32)),
            in_specs=[pl.BlockSpec(memory_space=pltpu.SMEM), any_spec] + [any_spec] * len(names),
            out_specs=(vmem, vmem),
            scratch_shapes=[pltpu.VMEM((n, w), f32)]
            + [pltpu.VMEM(s, f32) for s in shapes]
            + [pltpu.VMEM((8, n), f32), pltpu.VMEM((8, n // 2), f32), pltpu.VMEM((8, n), f32)]
            + [pltpu.VMEM((8 * R, n), f32), pltpu.VMEM((8 * C, n // 2), f32), pltpu.VMEM((8 * R, n), f32)]
            + [dma((len(names) + 1,)), dma((R,)), dma((R,)), dma((C,)), dma((C,)), dma((R,)), dma((R,))],
            compiler_params=pltpu.CompilerParams(
                collective_id=0, has_side_effects=True, vmem_limit_bytes=40 * 2**20
            ),
        )(ground_shift.reshape(1, 1), residual, *[jnp.asarray(v) for v in tables.values()])
        ratio = inner[0:1, 0:1] / previous.reshape(1, 1)
        return precond + ratio * direction, ratio.reshape(1)

    return jax.shard_map(
        body,
        mesh=mesh,
        in_specs=(P("row", "col"), P("row", "col"), P(), P()),
        out_specs=(P("row", "col"), P()),
        check_vma=False,
    )
```

```python
import functools
import jax
import jax.numpy as jnp
import numpy as np
from jax import lax
from jax.experimental import pallas as pl
from jax.experimental.pallas import tpu as pltpu
from jax.sharding import PartitionSpec as P

HI = lax.Precision.HIGHEST


def mm(a, b, ca=1, cb=0):
    return lax.dot_general(
        a[...], b[...], (((ca,), (cb,)), ((), ())), precision=HI, preferred_element_type=jnp.float32
    )


def dct_table(n):
    k = np.arange(n)[:, None]
    p = np.arange(n)[None, :]
    table = np.sqrt(2.0 / n) * np.cos(np.pi * (k * (2 * p + 1) % (4 * n)) / (2 * n))
    table[0] = np.sqrt(1.0 / n)
    return table


def edge_sines(blocks):
    e = np.arange(1, blocks)
    q = np.zeros((blocks, blocks))
    q[: blocks - 1, : blocks - 1] = np.sqrt(2.0 / blocks) * np.sin(
        np.pi * (np.outer(e, e) % (2 * blocks)) / blocks
    )
    return q


def make_tables(n, w, R, C):
    assert w == 2 * n and R % 2 == 0 and C <= R
    M = n // 2
    f = {}
    cn, cw = dct_table(n), dct_table(w)
    even = np.where(np.arange(n) % 2 == 0, 1.0, 0.0)
    phi, sgn = cn[:, 0], 2 * even - 1
    phj, sgj = cw[:, 0], np.where(np.arange(w) % 2 == 0, 1.0, -1.0)
    f["cw"], f["cn"] = cw, cn
    pk = np.zeros((32, w))
    pk[0], pk[1] = phj, sgj * phj
    pk[8:12], pk[12:16] = phj, sgj * phj
    pk[16] = 4 * np.sin(np.pi * np.arange(w) / (2 * w)) ** 2
    pk[17, :n] = 4 * np.sin(np.pi * np.arange(n) / (2 * n)) ** 2
    pk[18, :n], pk[19, :n] = even, 1 - even
    pk[24, :n], pk[25, :n] = phi, sgn * phi
    for i in range(8):
        pk[24 + i, n:] = phi * (even if i in (0, 1, 4, 5) else 1 - even)
    f["pk"] = pk
    s2 = np.zeros((R, 128))
    s2[:, 0] = np.sin(np.pi * np.arange(1, R + 1) / (2 * R)) ** 2
    s2[:C, 1] = np.sin(np.pi * np.arange(1, C + 1) / (2 * C)) ** 2
    f["s2"] = s2

    t = np.arange(R)[:, None]
    d = np.arange(R)[None, :]
    ang = np.pi * (t * d % (2 * R)) / R
    mix_c, mix_s = np.cos(ang), np.sin(ang)
    mix_s[0] = np.where(np.arange(R) % 2 == 0, 1.0, -1.0)
    q_r, q_c = edge_sines(R), edge_sines(C)
    shift_r, shift_c = np.zeros((R, R)), np.zeros((C, C))
    shift_r[1:], shift_c[1:] = q_r[:-1], q_c[:-1]

    qe = np.zeros((2, R, R, 8))
    for h in range(2):
        qe[h, :, :, h] = -shift_r.T
        qe[h, :, :, 2 + h] = q_r.T
    f["qe"] = qe.reshape(2 * R, 8 * R)
    qc = np.zeros((2 * C + 8, C, 8))
    for a in range(2):
        qc[a * C : (a + 1) * C, :, 2 * a] = -shift_c.T
        qc[a * C : (a + 1) * C, :, 2 * a + 1] = q_c.T
    qc[2 * C, :, 4] = 1.0
    f["qc"] = qc.reshape(2 * C + 8, 8 * C)
    alt = np.where(np.arange(R) % 2 == 0, 1.0, -1.0)[:, None]
    fold = lambda mix, sign: mix + sign * alt * mix[:, ::-1]
    nxt = lambda m: np.concatenate([m[:, 1:], np.zeros((R, 1))], axis=1)
    x3 = np.zeros((2, 2, R, R, 8))
    for side in range(2):
        for part, mix in ((0, mix_c), (2, mix_s)):
            ev, od = fold(mix, 1.0), fold(mix, -1.0)
            x3[0, side, :, :, part + side] = q_r.T @ (ev - nxt(ev)).T
            x3[1, side, :, :, part + side] = -q_r.T @ (od + nxt(od)).T
    f["x3"] = x3.reshape(4 * R, 8 * R)

    p = np.arange(n)[:, None]
    m = np.arange(M)[None, :]
    a_ang = np.pi * (m * (2 * p + 1) % (2 * n)) / n
    f["tab"] = np.concatenate([np.cos(a_ang), np.sin(a_ang)], axis=1)

    lanes = max(8 * R, n, 2 * M, 256)
    dev = np.zeros((R, 32, lanes))
    pos = 2 * np.arange(n) + 1
    N = n * R
    for r in range(R):
        nz = float(r > 0)
        for part, mix in ((0, mix_c), (1, mix_s)):
            for side in range(2):
                row = np.zeros((R, 8))
                row[:, 4 + side] = mix[r]
                dev[r, 2 * part + side, : 8 * R] = row.reshape(-1)
        for rep in range(2):
            for part, mix in ((0, mix_c), (1, mix_s)):
                top = mix[r] @ shift_r
                bot = -(mix[r] @ q_r)
                dev[r, 8 + 4 * rep + part, :R] = top + bot
                dev[r, 8 + 4 * rep + 2 + part, :R] = top - bot
        dev[r, 8, 128 : 128 + R] = shift_r[r]
        dev[r, 9, 128 : 128 + R] = -q_r[r]
        for base, sign in ((16, 1.0), (20, -1.0)):
            for side in range(2):
                row = np.zeros((R, 8))
                row[:, side] = fold(mix_c, sign)[:, r]
                row[:, 2 + side] = fold(mix_s, sign)[:, r]
                dev[r, base + side, : 8 * R] = row.reshape(-1)
        row = np.zeros((R, 8))
        row[:, 4] = 1.0
        dev[r, 18, : 8 * R] = row.reshape(-1)
        tau = (r, 2 * R - r if r > 0 else R)
        ca, sa = [], []
        for x in tau:
            b = np.pi * (x * pos % (4 * N)) / (2 * N)
            ca.append(np.cos(b))
            sa.append(np.sin(b))
        rot = [ca[0], -nz * sa[0], sa[0], nz * ca[0]]
        if r > 0:
            rot += [ca[1], sa[1], sa[1], -ca[1]]
        else:
            rot += [0 * pos, ca[1], 0 * pos, sa[1]]
        for i, v in enumerate(rot):
            dev[r, 24 + i, :n] = v
        k = np.concatenate([2 * R * np.arange(M) + x for x in tau])
        dev[r, 5, : 2 * M] = 4 * np.sin(np.pi * k / (2 * N)) ** 2
        dev[r, 6, : 2 * M] = np.where(k == 0, 1.0 / N, 2.0 / N)
    f["dev"] = dev
    devc = np.zeros((C, 8, 128))
    for c in range(C):
        devc[c, 0, :C] = shift_c[c]
        devc[c, 1, :C] = -q_c[c]
    f["devc"] = devc
    return {key: v.astype(np.float32) for key, v in f.items()}


def chain(mu, n):
    s = 0.5 * jnp.sqrt(mu)
    ch = jnp.sqrt(1.0 + s * s)
    x = s + s * s / (1.0 + ch)
    z = x / (2.0 + x)
    z2 = z * z
    acc = jnp.full_like(z, 1.0 / 19.0)
    for k in (17, 15, 13, 11, 9, 7, 5, 3, 1):
        acc = acc * z2 + 1.0 / k
    theta = 4.0 * z * acc
    decay = jnp.exp(-n * theta)
    shorter = jnp.exp(-(n - 1) * theta)
    diff = (ch - s) * (1.0 - shorter) / (2.0 * s * (1.0 + decay))
    far = ch * decay / (s * (1.0 - decay * decay))
    return 1.0 + 2.0 * diff, 4.0 * far


def split(x):
    high = x.astype(jnp.bfloat16)
    return high, (x - high.astype(jnp.float32)).astype(jnp.bfloat16)


def mm3(a, b):
    dot = lambda x, y: jnp.dot(x[...], y[...], preferred_element_type=jnp.float32)
    return dot(a[0], b[0]) + (dot(a[0], b[1]) + dot(a[1], b[0]))


def fold_lanes(x, width):
    out = x[:, :width]
    for i in range(1, x.shape[1] // width):
        out = out + x[:, i * width : (i + 1) * width]
    return out


MESH_ID = pl.DeviceIdType.MESH


def kernel(names, R, C, *refs):
    count = len(names)
    shift_ref, previous_ref, residual_ref, direction_ref = refs[:4]
    table_hbm = refs[4 : 4 + count]
    next_ref, ratio_ref = refs[4 + count : 6 + count]
    refs = refs[6 + count :]
    table_v, refs = refs[:count], refs[count:]
    (r_v, d_v, out1, out2, out3, buf1, buf2, buf3), refs = refs[:8], refs[8:]
    (spec_v, weight_v, yl_v, inv_v, cwh, cwl, cth, ctl), refs = refs[:8], refs[8:]
    load_sem, s1, v1, s2, v2, s3, v3 = refs
    row, col = lax.axis_index("row"), lax.axis_index("col")
    half = R // 2
    partner = row + 1 - 2 * lax.rem(row, 2)
    n, w = r_v.shape
    M = n // 2

    loads = {}
    for i, name in enumerate(names):
        src = table_hbm[i]
        if name == "dev":
            src = src.at[row]
        elif name == "devc":
            src = src.at[col]
        loads[name] = pltpu.make_async_copy(src, table_v[i], load_sem.at[i])
    loads["residual"] = pltpu.make_async_copy(residual_ref, r_v, load_sem.at[count])
    loads["direction"] = pltpu.make_async_copy(direction_ref, d_v, load_sem.at[count + 1])
    first = ("cw", "residual", "cn", "pk")
    rest = tuple(x for x in names if x not in first) + ("direction",)
    for name in first + rest:
        loads[name].start()

    barrier = pltpu.get_barrier_semaphore()

    @pl.loop(1, half)
    def _(i):
        peer = lax.rem(row + 2 * i, R)
        pl.semaphore_signal(barrier, inc=1, device_id=(peer, col), device_id_type=MESH_ID)

    @pl.loop(1, C)
    def _(i):
        peer = lax.rem(col + i, C)
        pl.semaphore_signal(barrier, inc=1, device_id=(row, peer), device_id_type=MESH_ID)

    pl.semaphore_signal(barrier, inc=1, device_id=(partner, col), device_id_type=MESH_ID)

    f = dict(zip(names, table_v))
    g = shift_ref[0]

    def tile(buf, slot):
        return buf.at[pl.ds(pl.multiple_of(slot * 8, 8), 8), :]

    def row_copy(src, buf, slot, send, recv, peer):
        return pltpu.make_async_remote_copy(
            src_ref=src,
            dst_ref=tile(buf, slot),
            send_sem=send,
            recv_sem=recv.at[slot],
            device_id=(peer, col),
            device_id_type=MESH_ID,
        )

    def row_start(out, buf, send, recv):
        @pl.loop(0, half - 1)
        def _(j):
            i = half // 2 + lax.div(j + 1, 2) * (1 - 2 * lax.rem(j, 2))
            row_copy(out, buf, row, send.at[i], recv, lax.rem(row + 2 * i, R)).start()

        row_copy(out, buf, row, send.at[0], recv, partner).start()
        buf[pl.ds(pl.multiple_of(row * 8, 8), 8), :] = out[...]

    def row_finish(out, buf, send, recv):
        @pl.loop(1, half)
        def _(i):
            slot = lax.rem(row + 2 * i, R)
            row_copy(out, buf, slot, send.at[0], recv, partner).wait_recv()
            row_copy(tile(buf, slot), buf, slot, send.at[half + i], recv, partner).start()

        @pl.loop(0, half)
        def _(i):
            slot = lax.rem(partner + 2 * i, R)
            row_copy(out, buf, slot, send.at[0], recv, partner).wait_recv()

    def row_drain(out, buf, send, recv):
        @pl.loop(0, half)
        def _(i):
            row_copy(out, buf, row, send.at[i], recv, partner).wait_send()

        @pl.loop(1, half)
        def _(i):
            row_copy(out, buf, row, send.at[half + i], recv, partner).wait_send()

    def col_copy(slot, peer):
        return pltpu.make_async_remote_copy(
            src_ref=out2,
            dst_ref=tile(buf2, slot),
            send_sem=s2.at[peer],
            recv_sem=v2.at[slot],
            device_id=(row, peer),
            device_id_type=MESH_ID,
        )

    loads["cw"].wait()
    loads["residual"].wait()
    half_way = mm(r_v, f["cw"], 1, 1)
    loads["cn"].wait()
    loads["pk"].wait()
    spec = mm(f["cn"], half_way)
    lams = f["pk"][16:24, :]
    lam_col = lams[:, :n].T[:, 1:2]
    weight = 1.0 / (lam_col + lams[0:1] + g)
    sol = weight * spec
    spec_v[...] = spec
    weight_v[...] = weight
    own_energy = fold_lanes(jnp.sum(spec * sol, axis=0, keepdims=True), M)
    p2 = f["pk"][0:8, :]
    p1 = f["pk"][24:32, :n]
    m8 = f["pk"][24:32, n:]
    zfl = mm(p1, sol)
    zb = mm(p2, sol, 1, 1)
    out1[...] = jnp.concatenate(
        [zfl[0:1, :n], zfl[0:1, n:], zfl[1:2, :n], zfl[1:2, n:], zb[0:4]], axis=0
    )
    pl.semaphore_wait(barrier, half + C - 1)
    row_start(out1, buf1, s1, v1)

    for name in rest:
        loads[name].wait()
    dev = f["dev"][...]
    base, far = chain(lams[0:1] + g, n)
    inv_v[...] = 1.0 / (base + far * f["s2"][...][:, 0:1])
    row_finish(out1, buf1, s1, v1)
    y2 = mm(f["qe"], buf1)
    mixed = mm(dev[0:8, : 8 * R], buf1)
    yl = jnp.concatenate([y2[:R], y2[R:]], axis=1)
    yl_v[...] = yl
    tl = yl * inv_v[...]
    energy_r = fold_lanes(jnp.sum(yl * tl, axis=0, keepdims=True), M)
    q8 = mm(dev[8:16, :R], tl) * f["pk"][8:16, :]
    v8 = mm(q8, weight_v, 1, 1) * m8
    z4 = jnp.concatenate(
        [
            mixed[0:1] + v8[0:1] + v8[2:3],
            mixed[1:2] + v8[4:5] + v8[6:7],
            mixed[2:3] + v8[1:2] + v8[3:4],
            mixed[3:4] + v8[5:6] + v8[7:8],
        ],
        axis=0,
    )
    zp = mm(z4, f["cn"])
    re, im = zp[0:2], zp[2:4]
    rot = dev[24:32, :n]
    a1 = re * rot[0:1] + im * rot[1:2]
    b1 = re * rot[2:3] + im * rot[3:4]
    a2 = re * rot[4:5] + im * rot[5:6]
    b2 = re * rot[6:7] + im * rot[7:8]
    yy = mm(jnp.concatenate([a1, a2, b1, b2], axis=0), f["tab"])
    y4 = yy[0:4, :M] - yy[4:8, M:]
    zero3 = jnp.zeros((3, M), jnp.float32)
    out2[...] = jnp.concatenate([y4, own_energy - energy_r * (1.0 / R), zero3], axis=0)

    @pl.loop(1, C)
    def _(i):
        peer = lax.rem(col + i, C)
        col_copy(col, peer).start()

    buf2[pl.ds(pl.multiple_of(col * 8, 8), 8), :] = out2[...]

    base, far = chain(dev[5:6, : 2 * M] + g, w)
    norm = dev[6:7, : 2 * M]
    inv_c = norm / (base + far * f["s2"][...][:C, 1:2])
    cwh[...], cwl[...] = split(f["cw"][...])
    cth[...], ctl[...] = split(f["cn"][...].T)

    @pl.loop(1, C)
    def _(i):
        peer = lax.rem(col + i, C)
        col_copy(peer, peer).wait_recv()

    y2 = mm(f["qc"], buf2)
    y = jnp.concatenate([y2[:C], y2[C : 2 * C]], axis=1)
    tl = y * inv_c
    energy = y2[2 * C : 2 * C + 1] - fold_lanes(jnp.sum(y * tl, axis=0, keepdims=True), M)
    q2 = mm(f["devc"][...][:, :C], tl)
    q4 = jnp.concatenate([q2[0:2, :M], q2[0:2, M:]], axis=0)
    u = mm(q4, f["tab"][:M, :M], 1, 1)
    v = mm(q4, f["tab"][:M, M:], 1, 1)
    rot = rot[:, :M]
    re = u[0:2] * rot[0:1] - v[0:2] * rot[2:3] + u[2:4] * rot[4:5] - v[2:4] * rot[6:7]
    im = u[0:2] * rot[1:2] - v[0:2] * rot[3:4] + u[2:4] * rot[5:6] - v[2:4] * rot[7:8]
    out3[...] = jnp.concatenate([re, im, energy, zero3], axis=0)
    row_start(out3, buf3, s3, v3)
    row_drain(out1, buf1, s1, v1)

    @pl.loop(1, C)
    def _(i):
        peer = lax.rem(col + i, C)
        col_copy(col, peer).wait_send()

    row_finish(out3, buf3, s3, v3)

    xx = mm(jnp.concatenate([f["x3"][...], dev[16:24, : 8 * R]], axis=0), buf3)
    inner = jnp.sum(xx[4 * R + 2 : 4 * R + 3])
    ratio = inner / previous_ref[0]
    xc = mm(xx, f["cn"][:, :M], 1, 1)
    moved = mm(xc[: 2 * R] * m8[0:1] + xc[2 * R : 4 * R] * m8[2:3], weight_v)
    y_all = yl_v[...] + moved[:R] * p2[0:1] + moved[R:] * p2[1:2]
    row_flux = mm(dev[8:16, 128 : 128 + R], y_all * inv_v[...])
    sides = xc[4 * R : 4 * R + 4] * lams[2:3, :n] + xc[4 * R + 4 :] * lams[3:4, :n]
    left = jnp.concatenate([p1[0:4], sides], axis=0)
    right = jnp.concatenate([row_flux[0:4], p2[0:4]], axis=0)
    sol = weight_v[...] * (spec_v[...] + mm(left.T, right))
    wide = mm3(split(sol), (cwh, cwl))
    precond = mm3((cth, ctl), split(wide))
    next_ref[...] = precond + ratio * d_v[...]
    ratio_ref[0] = ratio
    row_drain(out3, buf3, s3, v3)


def solution(mesh):
    R, C = mesh.shape["row"], mesh.shape["col"]

    def body(residual, direction, ground_shift, previous):
        n, w = residual.shape
        M = n // 2
        tables = make_tables(n, w, R, C)
        names = tuple(tables)
        shapes = [v.shape[1:] if k in ("dev", "devc") else v.shape for k, v in tables.items()]
        smem = pl.BlockSpec(memory_space=pltpu.SMEM)
        hbm = pl.BlockSpec(memory_space=pltpu.HBM)
        f32, bf16 = jnp.float32, jnp.bfloat16
        vm = lambda *shape: pltpu.VMEM(shape, f32)
        vb = lambda *shape: pltpu.VMEM(shape, bf16)
        dma = pltpu.SemaphoreType.DMA
        return pl.pallas_call(
            functools.partial(kernel, names, R, C),
            out_shape=(jax.ShapeDtypeStruct((n, w), f32), jax.ShapeDtypeStruct((1,), f32)),
            in_specs=[smem, smem] + [hbm] * (2 + len(names)),
            out_specs=(pl.BlockSpec(memory_space=pltpu.VMEM), smem),
            scratch_shapes=[pltpu.VMEM(s, f32) for s in shapes]
            + [vm(n, w), vm(n, w), vm(8, n), vm(8, M), vm(8, M)]
            + [vm(8 * R, n), vm(8 * C, M), vm(8 * R, M)]
            + [vm(n, w), vm(n, w), vm(R, w), vm(R, w), vb(w, w), vb(w, w), vb(n, n), vb(n, n)]
            + [dma((len(names) + 2,)), dma((R,)), dma((R,)), dma((C,)), dma((C,)), dma((R,)), dma((R,))],
            compiler_params=pltpu.CompilerParams(collective_id=0, has_side_effects=True),
        )(ground_shift, previous, residual, direction, *[jnp.asarray(v) for v in tables.values()])

    return jax.shard_map(
        body,
        mesh=mesh,
        in_specs=(P("row", "col"), P("row", "col"), P(), P()),
        out_specs=(P("row", "col"), P()),
        check_vma=False,
    )
```

```python
import functools
import jax
import jax.numpy as jnp
import numpy as np
from jax import lax
from jax.experimental import pallas as pl
from jax.experimental.pallas import tpu as pltpu
from jax.sharding import PartitionSpec as P

HI = lax.Precision.HIGHEST


def mm(a, b, ca=1, cb=0):
    return lax.dot_general(
        a[...], b[...], (((ca,), (cb,)), ((), ())), precision=HI, preferred_element_type=jnp.float32
    )


def dct_table(n):
    k = np.arange(n)[:, None]
    p = np.arange(n)[None, :]
    table = np.sqrt(2.0 / n) * np.cos(np.pi * (k * (2 * p + 1) % (4 * n)) / (2 * n))
    table[0] = np.sqrt(1.0 / n)
    return table


def edge_sines(blocks):
    e = np.arange(1, blocks)
    q = np.zeros((blocks, blocks))
    q[: blocks - 1, : blocks - 1] = np.sqrt(2.0 / blocks) * np.sin(
        np.pi * (np.outer(e, e) % (2 * blocks)) / blocks
    )
    return q


def make_tables(n, w, R, C):
    assert w == 2 * n and R % 2 == 0 and C <= R
    M = n // 2
    f = {}
    cn, cw = dct_table(n), dct_table(w)
    even = np.where(np.arange(n) % 2 == 0, 1.0, 0.0)
    phi, sgn = cn[:, 0], 2 * even - 1
    phj, sgj = cw[:, 0], np.where(np.arange(w) % 2 == 0, 1.0, -1.0)
    f["cw"], f["cn"] = cw, cn
    pk = np.zeros((32, w))
    pk[0], pk[1] = phj, sgj * phj
    pk[8:12], pk[12:16] = phj, sgj * phj
    pk[16] = 4 * np.sin(np.pi * np.arange(w) / (2 * w)) ** 2
    pk[17, :n] = 4 * np.sin(np.pi * np.arange(n) / (2 * n)) ** 2
    pk[18, :n], pk[19, :n] = even, 1 - even
    pk[24, :n], pk[25, :n] = phi, sgn * phi
    for i in range(8):
        pk[24 + i, n:] = phi * (even if i in (0, 1, 4, 5) else 1 - even)
    f["pk"] = pk
    s2 = np.zeros((R, 128))
    s2[:, 0] = np.sin(np.pi * np.arange(1, R + 1) / (2 * R)) ** 2
    s2[:C, 1] = np.sin(np.pi * np.arange(1, C + 1) / (2 * C)) ** 2
    f["s2"] = s2

    t = np.arange(R)[:, None]
    d = np.arange(R)[None, :]
    ang = np.pi * (t * d % (2 * R)) / R
    mix_c, mix_s = np.cos(ang), np.sin(ang)
    mix_s[0] = np.where(np.arange(R) % 2 == 0, 1.0, -1.0)
    q_r, q_c = edge_sines(R), edge_sines(C)
    shift_r, shift_c = np.zeros((R, R)), np.zeros((C, C))
    shift_r[1:], shift_c[1:] = q_r[:-1], q_c[:-1]

    qe = np.zeros((2, R, R, 8))
    for h in range(2):
        qe[h, :, :, h] = -shift_r.T
        qe[h, :, :, 2 + h] = q_r.T
    f["qe"] = qe.reshape(2 * R, 8 * R)
    qc = np.zeros((2 * C + 8, C, 8))
    for a in range(2):
        qc[a * C : (a + 1) * C, :, 2 * a] = -shift_c.T
        qc[a * C : (a + 1) * C, :, 2 * a + 1] = q_c.T
    qc[2 * C, :, 4] = 1.0
    f["qc"] = qc.reshape(2 * C + 8, 8 * C)
    alt = np.where(np.arange(R) % 2 == 0, 1.0, -1.0)[:, None]
    fold = lambda mix, sign: mix + sign * alt * mix[:, ::-1]
    nxt = lambda m: np.concatenate([m[:, 1:], np.zeros((R, 1))], axis=1)
    x3 = np.zeros((2, 2, R, R, 8))
    for side in range(2):
        for part, mix in ((0, mix_c), (2, mix_s)):
            ev, od = fold(mix, 1.0), fold(mix, -1.0)
            x3[0, side, :, :, part + side] = q_r.T @ (ev - nxt(ev)).T
            x3[1, side, :, :, part + side] = -q_r.T @ (od + nxt(od)).T
    f["x3"] = x3.reshape(4 * R, 8 * R)

    p = np.arange(n)[:, None]
    m = np.arange(M)[None, :]
    a_ang = np.pi * (m * (2 * p + 1) % (2 * n)) / n
    f["tab"] = np.concatenate([np.cos(a_ang), np.sin(a_ang)], axis=1)

    lanes = max(8 * R, n, 2 * M, 256)
    dev = np.zeros((R, 32, lanes))
    pos = 2 * np.arange(n) + 1
    N = n * R
    for r in range(R):
        nz = float(r > 0)
        for part, mix in ((0, mix_c), (1, mix_s)):
            for side in range(2):
                row = np.zeros((R, 8))
                row[:, 4 + side] = mix[r]
                dev[r, 2 * part + side, : 8 * R] = row.reshape(-1)
        for rep in range(2):
            for part, mix in ((0, mix_c), (1, mix_s)):
                top = mix[r] @ shift_r
                bot = -(mix[r] @ q_r)
                dev[r, 8 + 4 * rep + part, :R] = top + bot
                dev[r, 8 + 4 * rep + 2 + part, :R] = top - bot
        dev[r, 8, 128 : 128 + R] = shift_r[r]
        dev[r, 9, 128 : 128 + R] = -q_r[r]
        for base, sign in ((16, 1.0), (20, -1.0)):
            for side in range(2):
                row = np.zeros((R, 8))
                row[:, side] = fold(mix_c, sign)[:, r]
                row[:, 2 + side] = fold(mix_s, sign)[:, r]
                dev[r, base + side, : 8 * R] = row.reshape(-1)
        row = np.zeros((R, 8))
        row[:, 4] = 1.0
        dev[r, 18, : 8 * R] = row.reshape(-1)
        tau = (r, 2 * R - r if r > 0 else R)
        ca, sa = [], []
        for x in tau:
            b = np.pi * (x * pos % (4 * N)) / (2 * N)
            ca.append(np.cos(b))
            sa.append(np.sin(b))
        rot = [ca[0], -nz * sa[0], sa[0], nz * ca[0]]
        if r > 0:
            rot += [ca[1], sa[1], sa[1], -ca[1]]
        else:
            rot += [0 * pos, ca[1], 0 * pos, sa[1]]
        for i, v in enumerate(rot):
            dev[r, 24 + i, :n] = v
        k = np.concatenate([2 * R * np.arange(M) + x for x in tau])
        dev[r, 5, : 2 * M] = 4 * np.sin(np.pi * k / (2 * N)) ** 2
        dev[r, 6, : 2 * M] = np.where(k == 0, 1.0 / N, 2.0 / N)
    f["dev"] = dev
    devc = np.zeros((C, 8, 128))
    for c in range(C):
        devc[c, 0, :C] = shift_c[c]
        devc[c, 1, :C] = -q_c[c]
    f["devc"] = devc
    return {key: v.astype(np.float32) for key, v in f.items()}


def chain(mu, n):
    s = 0.5 * jnp.sqrt(mu)
    ch = jnp.sqrt(1.0 + s * s)
    x = s + s * s / (1.0 + ch)
    z = x / (2.0 + x)
    z2 = z * z
    acc = jnp.full_like(z, 1.0 / 19.0)
    for k in (17, 15, 13, 11, 9, 7, 5, 3, 1):
        acc = acc * z2 + 1.0 / k
    theta = 4.0 * z * acc
    decay = jnp.exp(-n * theta)
    shorter = jnp.exp(-(n - 1) * theta)
    diff = (ch - s) * (1.0 - shorter) / (2.0 * s * (1.0 + decay))
    far = ch * decay / (s * (1.0 - decay * decay))
    return 1.0 + 2.0 * diff, 4.0 * far


def split(x):
    high = x.astype(jnp.bfloat16)
    return high, (x - high.astype(jnp.float32)).astype(jnp.bfloat16)


def mm3(a, b):
    dot = lambda x, y: jnp.dot(x[...], y[...], preferred_element_type=jnp.float32)
    return dot(a[0], b[0]) + (dot(a[0], b[1]) + dot(a[1], b[0]))


def fold_lanes(x, width):
    out = x[:, :width]
    for i in range(1, x.shape[1] // width):
        out = out + x[:, i * width : (i + 1) * width]
    return out


MESH_ID = pl.DeviceIdType.MESH


def kernel(names, R, C, *refs):
    count = len(names)
    scalar_ref, residual_ref = refs[:2]
    table_hbm = refs[2 : 2 + count]
    next_ref, inner_ref = refs[2 + count : 4 + count]
    refs = refs[4 + count :]
    table_v, refs = refs[:count], refs[count:]
    (r_v, out1, out2, out3, buf1, buf2, buf3), refs = refs[:7], refs[7:]
    (spec_v, weight_v, yl_v, inv_v, cwh, cwl, cth, ctl), refs = refs[:8], refs[8:]
    load_sem, s1, v1, s2, v2, s3, v3 = refs
    row, col = lax.axis_index("row"), lax.axis_index("col")
    half = R // 2
    partner = row + 1 - 2 * lax.rem(row, 2)
    n, w = r_v.shape
    M = n // 2

    loads = {}
    for i, name in enumerate(names):
        src = table_hbm[i]
        if name == "dev":
            src = src.at[row]
        elif name == "devc":
            src = src.at[col]
        loads[name] = pltpu.make_async_copy(src, table_v[i], load_sem.at[i])
    loads["residual"] = pltpu.make_async_copy(residual_ref, r_v, load_sem.at[count])
    first = ("cw", "residual", "cn", "pk")
    rest = tuple(x for x in names if x not in first)
    for name in first + rest:
        loads[name].start()

    barrier = pltpu.get_barrier_semaphore()

    @pl.loop(1, half)
    def _(i):
        peer = lax.rem(row + 2 * i, R)
        pl.semaphore_signal(barrier, inc=1, device_id=(peer, col), device_id_type=MESH_ID)

    @pl.loop(1, C)
    def _(i):
        peer = lax.rem(col + i, C)
        pl.semaphore_signal(barrier, inc=1, device_id=(row, peer), device_id_type=MESH_ID)

    pl.semaphore_signal(barrier, inc=1, device_id=(partner, col), device_id_type=MESH_ID)

    f = dict(zip(names, table_v))
    g = scalar_ref[0:1, 0:1]

    def tile(buf, slot):
        return buf.at[pl.ds(pl.multiple_of(slot * 8, 8), 8), :]

    def row_copy(src, buf, slot, send, recv, peer):
        return pltpu.make_async_remote_copy(
            src_ref=src,
            dst_ref=tile(buf, slot),
            send_sem=send,
            recv_sem=recv.at[slot],
            device_id=(peer, col),
            device_id_type=MESH_ID,
        )

    def row_start(out, buf, send, recv):
        @pl.loop(0, half - 1)
        def _(j):
            i = half // 2 + lax.div(j + 1, 2) * (1 - 2 * lax.rem(j, 2))
            row_copy(out, buf, row, send.at[i], recv, lax.rem(row + 2 * i, R)).start()

        row_copy(out, buf, row, send.at[0], recv, partner).start()
        buf[pl.ds(pl.multiple_of(row * 8, 8), 8), :] = out[...]

    def row_finish(out, buf, send, recv):
        @pl.loop(1, half)
        def _(i):
            slot = lax.rem(row + 2 * i, R)
            row_copy(out, buf, slot, send.at[0], recv, partner).wait_recv()
            row_copy(tile(buf, slot), buf, slot, send.at[half + i], recv, partner).start()

        @pl.loop(0, half)
        def _(i):
            slot = lax.rem(partner + 2 * i, R)
            row_copy(out, buf, slot, send.at[0], recv, partner).wait_recv()

    def row_drain(out, buf, send, recv):
        @pl.loop(0, half)
        def _(i):
            row_copy(out, buf, row, send.at[i], recv, partner).wait_send()

        @pl.loop(1, half)
        def _(i):
            row_copy(out, buf, row, send.at[half + i], recv, partner).wait_send()

    def col_copy(slot, peer):
        return pltpu.make_async_remote_copy(
            src_ref=out2,
            dst_ref=tile(buf2, slot),
            send_sem=s2.at[peer],
            recv_sem=v2.at[slot],
            device_id=(row, peer),
            device_id_type=MESH_ID,
        )

    loads["cw"].wait()
    loads["residual"].wait()
    half_way = mm(r_v, f["cw"], 1, 1)
    loads["cn"].wait()
    loads["pk"].wait()
    spec = mm(f["cn"], half_way)
    lams = f["pk"][16:24, :]
    lam_col = lams[:, :n].T[:, 1:2]
    weight = 1.0 / (lam_col + lams[0:1] + g)
    sol = weight * spec
    spec_v[...] = spec
    weight_v[...] = weight
    own_energy = fold_lanes(jnp.sum(spec * sol, axis=0, keepdims=True), M)
    p2 = f["pk"][0:8, :]
    p1 = f["pk"][24:32, :n]
    m8 = f["pk"][24:32, n:]
    zfl = mm(p1, sol)
    zb = mm(p2, sol, 1, 1)
    out1[...] = jnp.concatenate(
        [zfl[0:1, :n], zfl[0:1, n:], zfl[1:2, :n], zfl[1:2, n:], zb[0:4]], axis=0
    )
    pl.semaphore_wait(barrier, half + C - 1)
    row_start(out1, buf1, s1, v1)

    for name in rest:
        loads[name].wait()
    dev = f["dev"][...]
    base, far = chain(lams[0:1] + g, n)
    inv_v[...] = 1.0 / (base + far * f["s2"][...][:, 0:1])
    row_finish(out1, buf1, s1, v1)
    y2 = mm(f["qe"], buf1)
    mixed = mm(dev[0:8, : 8 * R], buf1)
    yl = jnp.concatenate([y2[:R], y2[R:]], axis=1)
    yl_v[...] = yl
    tl = yl * inv_v[...]
    energy_r = fold_lanes(jnp.sum(yl * tl, axis=0, keepdims=True), M)
    q8 = mm(dev[8:16, :R], tl) * f["pk"][8:16, :]
    v8 = mm(q8, weight_v, 1, 1) * m8
    z4 = jnp.concatenate(
        [
            mixed[0:1] + v8[0:1] + v8[2:3],
            mixed[1:2] + v8[4:5] + v8[6:7],
            mixed[2:3] + v8[1:2] + v8[3:4],
            mixed[3:4] + v8[5:6] + v8[7:8],
        ],
        axis=0,
    )
    zp = mm(z4, f["cn"])
    re, im = zp[0:2], zp[2:4]
    rot = dev[24:32, :n]
    a1 = re * rot[0:1] + im * rot[1:2]
    b1 = re * rot[2:3] + im * rot[3:4]
    a2 = re * rot[4:5] + im * rot[5:6]
    b2 = re * rot[6:7] + im * rot[7:8]
    yy = mm(jnp.concatenate([a1, a2, b1, b2], axis=0), f["tab"])
    y4 = yy[0:4, :M] - yy[4:8, M:]
    zero3 = jnp.zeros((3, M), jnp.float32)
    out2[...] = jnp.concatenate([y4, own_energy - energy_r * (1.0 / R), zero3], axis=0)

    @pl.loop(1, C)
    def _(i):
        peer = lax.rem(col + i, C)
        col_copy(col, peer).start()

    buf2[pl.ds(pl.multiple_of(col * 8, 8), 8), :] = out2[...]

    base, far = chain(dev[5:6, : 2 * M] + g, w)
    norm = dev[6:7, : 2 * M]
    inv_c = norm / (base + far * f["s2"][...][:C, 1:2])
    cwh[...], cwl[...] = split(f["cw"][...])
    cth[...], ctl[...] = split(f["cn"][...].T)

    @pl.loop(1, C)
    def _(i):
        peer = lax.rem(col + i, C)
        col_copy(peer, peer).wait_recv()

    y2 = mm(f["qc"], buf2)
    y = jnp.concatenate([y2[:C], y2[C : 2 * C]], axis=1)
    tl = y * inv_c
    energy = y2[2 * C : 2 * C + 1] - fold_lanes(jnp.sum(y * tl, axis=0, keepdims=True), M)
    q2 = mm(f["devc"][...][:, :C], tl)
    q4 = jnp.concatenate([q2[0:2, :M], q2[0:2, M:]], axis=0)
    u = mm(q4, f["tab"][:M, :M], 1, 1)
    v = mm(q4, f["tab"][:M, M:], 1, 1)
    rot = rot[:, :M]
    re = u[0:2] * rot[0:1] - v[0:2] * rot[2:3] + u[2:4] * rot[4:5] - v[2:4] * rot[6:7]
    im = u[0:2] * rot[1:2] - v[0:2] * rot[3:4] + u[2:4] * rot[5:6] - v[2:4] * rot[7:8]
    out3[...] = jnp.concatenate([re, im, energy, zero3], axis=0)
    row_start(out3, buf3, s3, v3)
    row_drain(out1, buf1, s1, v1)

    @pl.loop(1, C)
    def _(i):
        peer = lax.rem(col + i, C)
        col_copy(col, peer).wait_send()

    row_finish(out3, buf3, s3, v3)

    xx = mm(jnp.concatenate([f["x3"][...], dev[16:24, : 8 * R]], axis=0), buf3)
    inner = jnp.sum(xx[4 * R + 2 : 4 * R + 3], axis=1, keepdims=True)
    xc = mm(xx, f["cn"][:, :M], 1, 1)
    moved = mm(xc[: 2 * R] * m8[0:1] + xc[2 * R : 4 * R] * m8[2:3], weight_v)
    y_all = yl_v[...] + moved[:R] * p2[0:1] + moved[R:] * p2[1:2]
    row_flux = mm(dev[8:16, 128 : 128 + R], y_all * inv_v[...])
    sides = xc[4 * R : 4 * R + 4] * lams[2:3, :n] + xc[4 * R + 4 :] * lams[3:4, :n]
    left = jnp.concatenate([p1[0:4], sides], axis=0)
    right = jnp.concatenate([row_flux[0:4], p2[0:4]], axis=0)
    sol = weight_v[...] * (spec_v[...] + mm(left.T, right))
    wide = mm3(split(sol), (cwh, cwl))
    precond = mm3((cth, ctl), split(wide))
    next_ref[...] = precond
    inner_ref[...] = jnp.broadcast_to(inner, inner_ref.shape)
    row_drain(out3, buf3, s3, v3)


def finish(scalar_ref, inner_ref, precond_ref, direction_ref, next_ref, ratio_ref):
    ratio = inner_ref[0:1, 0:1] / scalar_ref[1:2, 0:1]
    next_ref[...] = precond_ref[...] + ratio * direction_ref[...]
    ratio_ref[0] = jnp.sum(ratio)


def solution(mesh):
    R, C = mesh.shape["row"], mesh.shape["col"]

    def body(residual, direction, ground_shift, previous):
        n, w = residual.shape
        M = n // 2
        tables = make_tables(n, w, R, C)
        names = tuple(tables)
        shapes = [v.shape[1:] if k in ("dev", "devc") else v.shape for k, v in tables.items()]
        smem = pl.BlockSpec(memory_space=pltpu.SMEM)
        hbm = pl.BlockSpec(memory_space=pltpu.HBM)
        f32, bf16 = jnp.float32, jnp.bfloat16
        vm = lambda *shape: pltpu.VMEM(shape, f32)
        vb = lambda *shape: pltpu.VMEM(shape, bf16)
        dma = pltpu.SemaphoreType.DMA
        vmem = pl.BlockSpec(memory_space=pltpu.VMEM)
        held = lambda x: pltpu.with_memory_space_constraint(x, pltpu.HBM)
        lane = lax.broadcasted_iota(jnp.int32, (8, 128), 0)
        scalars = jnp.where(lane == 0, ground_shift, previous)
        precond, inner = pl.pallas_call(
            functools.partial(kernel, names, R, C),
            out_shape=(jax.ShapeDtypeStruct((n, w), f32), jax.ShapeDtypeStruct((8, 128), f32)),
            in_specs=[vmem] + [hbm] * (1 + len(names)),
            out_specs=(vmem, vmem),
            scratch_shapes=[pltpu.VMEM(s, f32) for s in shapes]
            + [vm(n, w), vm(8, n), vm(8, M), vm(8, M)]
            + [vm(8 * R, n), vm(8 * C, M), vm(8 * R, M)]
            + [vm(n, w), vm(n, w), vm(R, w), vm(R, w), vb(w, w), vb(w, w), vb(n, n), vb(n, n)]
            + [dma((len(names) + 1,)), dma((R,)), dma((R,)), dma((C,)), dma((C,)), dma((R,)), dma((R,))],
            compiler_params=pltpu.CompilerParams(
                collective_id=0, has_side_effects=True, vmem_limit_bytes=24 * 2**20
            ),
        )(scalars, held(residual), *[held(jnp.asarray(v)) for v in tables.values()])
        return pl.pallas_call(
            finish,
            out_shape=(jax.ShapeDtypeStruct((n, w), f32), jax.ShapeDtypeStruct((1,), f32)),
            in_specs=[vmem] * 4,
            out_specs=(vmem, smem),
            compiler_params=pltpu.CompilerParams(vmem_limit_bytes=8 * 2**20),
        )(scalars, inner, precond, direction)

    return jax.shard_map(
        body,
        mesh=mesh,
        in_specs=(P("row", "col"), P("row", "col"), P(), P()),
        out_specs=(P("row", "col"), P()),
        check_vma=False,
    )
```

```python
import functools
import jax
import jax.numpy as jnp
import numpy as np
from jax import lax
from jax.experimental import pallas as pl
from jax.experimental.pallas import tpu as pltpu
from jax.sharding import PartitionSpec as P

HI = lax.Precision.HIGHEST
FAR1 = 1
FAR3 = 1


def mm(a, b, ca=1, cb=0):
    return lax.dot_general(
        a[...], b[...], (((ca,), (cb,)), ((), ())), precision=HI, preferred_element_type=jnp.float32
    )


def dct_table(n):
    k = np.arange(n)[:, None]
    p = np.arange(n)[None, :]
    table = np.sqrt(2.0 / n) * np.cos(np.pi * (k * (2 * p + 1) % (4 * n)) / (2 * n))
    table[0] = np.sqrt(1.0 / n)
    return table


def edge_sines(blocks):
    e = np.arange(1, blocks)
    q = np.zeros((blocks, blocks))
    q[: blocks - 1, : blocks - 1] = np.sqrt(2.0 / blocks) * np.sin(
        np.pi * (np.outer(e, e) % (2 * blocks)) / blocks
    )
    return q


def stack6(a):
    cut = lambda x: x.astype(np.float32).astype(jnp.bfloat16).astype(np.float64)
    high = cut(a)
    mid = cut(a - high)
    low = cut(a - high - mid)
    return np.concatenate([high, mid, low, high, mid, high], axis=-1)


def make_tables(n, w, R, C):
    assert w == 2 * n and R % 2 == 0 and C <= R
    M = n // 2
    f = {}
    cn, cw = dct_table(n), dct_table(w)
    even = np.where(np.arange(n) % 2 == 0, 1.0, 0.0)
    phi, sgn = cn[:, 0], 2 * even - 1
    phj, sgj = cw[:, 0], np.where(np.arange(w) % 2 == 0, 1.0, -1.0)
    f["cw"], f["cn"] = cw, cn
    pk = np.zeros((32, w))
    pk[0], pk[1] = phj, sgj * phj
    pk[8:12], pk[12:16] = phj, sgj * phj
    pk[16] = 4 * np.sin(np.pi * np.arange(w) / (2 * w)) ** 2
    pk[17, :n] = 4 * np.sin(np.pi * np.arange(n) / (2 * n)) ** 2
    pk[18, :n], pk[19, :n] = even, 1 - even
    pk[24, :n], pk[25, :n] = phi, sgn * phi
    for i in range(8):
        pk[24 + i, n:] = phi * (even if i in (0, 1, 4, 5) else 1 - even)
    f["pk"] = pk
    s2 = np.zeros((R, 128))
    s2[:, 0] = np.sin(np.pi * np.arange(1, R + 1) / (2 * R)) ** 2
    s2[:C, 1] = np.sin(np.pi * np.arange(1, C + 1) / (2 * C)) ** 2
    f["s2"] = s2

    t = np.arange(R)[:, None]
    d = np.arange(R)[None, :]
    ang = np.pi * (t * d % (2 * R)) / R
    mix_c, mix_s = np.cos(ang), np.sin(ang)
    mix_s[0] = np.where(np.arange(R) % 2 == 0, 1.0, -1.0)
    q_r, q_c = edge_sines(R), edge_sines(C)
    shift_r, shift_c = np.zeros((R, R)), np.zeros((C, C))
    shift_r[1:], shift_c[1:] = q_r[:-1], q_c[:-1]

    qe = np.zeros((2, R, R, 8))
    for h in range(2):
        qe[h, :, :, h] = -shift_r.T
        qe[h, :, :, 2 + h] = q_r.T
    f["qe"] = qe.reshape(2 * R, 8 * R)
    qc = np.zeros((2 * C + 8, C, 8))
    for a in range(2):
        qc[a * C : (a + 1) * C, :, 2 * a] = -shift_c.T
        qc[a * C : (a + 1) * C, :, 2 * a + 1] = q_c.T
    qc[2 * C, :, 4] = 1.0
    f["qc"] = qc.reshape(2 * C + 8, 8 * C)
    alt = np.where(np.arange(R) % 2 == 0, 1.0, -1.0)[:, None]
    fold = lambda mix, sign: mix + sign * alt * mix[:, ::-1]
    nxt = lambda m: np.concatenate([m[:, 1:], np.zeros((R, 1))], axis=1)
    x3 = np.zeros((2, 2, R, R, 8))
    for side in range(2):
        for part, mix in ((0, mix_c), (2, mix_s)):
            ev, od = fold(mix, 1.0), fold(mix, -1.0)
            x3[0, side, :, :, part + side] = q_r.T @ (ev - nxt(ev)).T
            x3[1, side, :, :, part + side] = -q_r.T @ (od + nxt(od)).T
    f["x3"] = x3.reshape(4 * R, 8 * R)

    p = np.arange(n)[:, None]
    m = np.arange(M)[None, :]
    a_ang = np.pi * (m * (2 * p + 1) % (2 * n)) / n
    f["tab"] = np.concatenate([np.cos(a_ang), np.sin(a_ang)], axis=1)

    lanes = max(8 * R, n, 2 * M, 256)
    dev = np.zeros((R, 40, lanes))
    pos = 2 * np.arange(n) + 1
    N = n * R
    for r in range(R):
        nz = float(r > 0)
        for part, mix in ((0, mix_c), (1, mix_s)):
            for side in range(2):
                row = np.zeros((R, 8))
                row[:, 4 + side] = mix[r]
                dev[r, 2 * part + side, : 8 * R] = row.reshape(-1)
        for rep in range(2):
            for part, mix in ((0, mix_c), (1, mix_s)):
                top = mix[r] @ shift_r
                bot = -(mix[r] @ q_r)
                dev[r, 8 + 4 * rep + part, : 6 * R] = stack6(top + bot)
                dev[r, 8 + 4 * rep + 2 + part, : 6 * R] = stack6(top - bot)
        dev[r, 32, : 6 * R] = stack6(shift_r[r])
        dev[r, 33, : 6 * R] = stack6(-q_r[r])
        for base, sign in ((16, 1.0), (20, -1.0)):
            for side in range(2):
                row = np.zeros((R, 8))
                row[:, side] = fold(mix_c, sign)[:, r]
                row[:, 2 + side] = fold(mix_s, sign)[:, r]
                dev[r, base + side, : 8 * R] = row.reshape(-1)
        row = np.zeros((R, 8))
        row[:, 4] = 1.0
        dev[r, 18, : 8 * R] = row.reshape(-1)
        tau = (r, 2 * R - r if r > 0 else R)
        ca, sa = [], []
        for x in tau:
            b = np.pi * (x * pos % (4 * N)) / (2 * N)
            ca.append(np.cos(b))
            sa.append(np.sin(b))
        rot = [ca[0], -nz * sa[0], sa[0], nz * ca[0]]
        if r > 0:
            rot += [ca[1], sa[1], sa[1], -ca[1]]
        else:
            rot += [0 * pos, ca[1], 0 * pos, sa[1]]
        for i, v in enumerate(rot):
            dev[r, 24 + i, :n] = v
        k = np.concatenate([2 * R * np.arange(M) + x for x in tau])
        dev[r, 5, : 2 * M] = 4 * np.sin(np.pi * k / (2 * N)) ** 2
        dev[r, 6, : 2 * M] = np.where(k == 0, 1.0 / N, 2.0 / N)
    f["dev"] = dev
    devc = np.zeros((C, 8, 128))
    for c in range(C):
        devc[c, 0, : 6 * C] = stack6(shift_c[c])
        devc[c, 1, : 6 * C] = stack6(-q_c[c])
    f["devc"] = devc
    return {key: v.astype(np.float32) for key, v in f.items()}


def chain(mu, n):
    s = 0.5 * jnp.sqrt(mu)
    ch = jnp.sqrt(1.0 + s * s)
    x = s + s * s / (1.0 + ch)
    z = x / (2.0 + x)
    z2 = z * z
    acc = jnp.full_like(z, 1.0 / 19.0)
    for k in (17, 15, 13, 11, 9, 7, 5, 3, 1):
        acc = acc * z2 + 1.0 / k
    theta = 4.0 * z * acc
    decay = jnp.exp(-n * theta)
    shorter = jnp.exp(-(n - 1) * theta)
    diff = (ch - s) * (1.0 - shorter) / (2.0 * s * (1.0 + decay))
    far = ch * decay / (s * (1.0 - decay * decay))
    return 1.0 + 2.0 * diff, 4.0 * far


def split(x):
    high = x.astype(jnp.bfloat16)
    return high, (x - high.astype(jnp.float32)).astype(jnp.bfloat16)


def mm3(a, b):
    dot = lambda x, y: jnp.dot(x[...], y[...], preferred_element_type=jnp.float32)
    return dot(a[0], b[0]) + (dot(a[0], b[1]) + dot(a[1], b[0]))


def split3(x):
    high = x.astype(jnp.bfloat16).astype(jnp.float32)
    rest = x - high
    mid = rest.astype(jnp.bfloat16).astype(jnp.float32)
    return high, mid, rest - mid


def store3(refs, x):
    for ref, part in zip(refs, split3(x)):
        ref[...] = part.astype(jnp.bfloat16)


def mm6(a, b, ca=1, cb=0):
    rows = a.shape[0]
    a3 = jnp.concatenate(split3(a), axis=0).astype(jnp.bfloat16)
    dot = lambda x, y: lax.dot_general(
        x, y[...], (((ca,), (cb,)), ((), ())), preferred_element_type=jnp.float32
    )
    p0, p1, p2 = dot(a3, b[0]), dot(a3[: 2 * rows], b[1]), dot(a3[: 2 * rows], b[2])
    low = p0[2 * rows :] + p1[rows:] + p2[:rows]
    return p0[:rows] + (p0[rows : 2 * rows] + p1[:rows] + low)


def tall6(b):
    high, mid, low = split3(b)
    return jnp.concatenate([high, high, high, mid, mid, low], axis=0).astype(jnp.bfloat16)


def fold_lanes(x, width):
    out = x[:, :width]
    for i in range(1, x.shape[1] // width):
        out = out + x[:, i * width : (i + 1) * width]
    return out


MESH_ID = pl.DeviceIdType.MESH


def kernel(names, R, C, *refs):
    count = len(names)
    scalar_ref, residual_ref = refs[:2]
    table_hbm = refs[2 : 2 + count]
    next_ref, inner_ref = refs[2 + count : 4 + count]
    refs = refs[4 + count :]
    table_v, refs = refs[:count], refs[count:]
    (r_v, out1, out2, out3, buf1, buf2, buf3), refs = refs[:7], refs[7:]
    (spec_v, weight_v, yl_v, inv_v, cwh, cwl, cth, ctl), refs = refs[:8], refs[8:]
    w3, c3, t3, refs = refs[:3], refs[3:6], refs[6:9], refs[9:]
    load_sem, s1, v1, o1, s2, v2, s3, v3, o3 = refs
    row, col = lax.axis_index("row"), lax.axis_index("col")
    half = R // 2
    partner = row + 1 - 2 * lax.rem(row, 2)
    n, w = r_v.shape
    M = n // 2
    far1, far3 = min(FAR1, half - 1), min(FAR3, half - 1)
    far_most = max(far1, far3)

    def chip_step(j):
        return half // 2 + lax.div(j + 1, 2) * (1 - 2 * lax.rem(j, 2))


    loads = {}
    for i, name in enumerate(names):
        src = table_hbm[i]
        if name == "dev":
            src = src.at[row]
        elif name == "devc":
            src = src.at[col]
        loads[name] = pltpu.make_async_copy(src, table_v[i], load_sem.at[i])
    loads["residual"] = pltpu.make_async_copy(residual_ref, r_v, load_sem.at[count])
    first = ("cn", "residual", "cw", "pk")
    rest = tuple(x for x in names if x not in first)
    for name in first + rest:
        loads[name].start()

    barrier = pltpu.get_barrier_semaphore()

    @pl.loop(1, half)
    def _(i):
        peer = lax.rem(row + 2 * i, R)
        pl.semaphore_signal(barrier, inc=1, device_id=(peer, col), device_id_type=MESH_ID)

    @pl.loop(1, C)
    def _(i):
        peer = lax.rem(col + i, C)
        pl.semaphore_signal(barrier, inc=1, device_id=(row, peer), device_id_type=MESH_ID)

    @pl.loop(0, far_most)
    def _(j):
        peer = lax.rem(partner + 2 * chip_step(j), R)
        pl.semaphore_signal(barrier, inc=1, device_id=(peer, col), device_id_type=MESH_ID)

    pl.semaphore_signal(barrier, inc=1, device_id=(partner, col), device_id_type=MESH_ID)

    f = dict(zip(names, table_v))
    g = scalar_ref[0:1, 0:1]

    def tile(buf, slot):
        return buf.at[pl.ds(pl.multiple_of(slot * 8, 8), 8), :]

    def row_copy(src, buf, slot, send, recv, peer):
        return pltpu.make_async_remote_copy(
            src_ref=src,
            dst_ref=tile(buf, slot),
            send_sem=send,
            recv_sem=recv,
            device_id=(peer, col),
            device_id_type=MESH_ID,
        )

    def wait_tiles(buf, tiles, sem):
        part = buf.at[pl.ds(0, tiles * 8), :]
        pltpu.make_async_copy(part, part, sem).wait()

    def row_start(out, buf, send, same, other, far_both):
        @pl.loop(0, far_both)
        def _(j):
            i = chip_step(j)
            chip = lax.div(row, 2)
            row_copy(out, buf, row, send, same.at[chip], lax.rem(row + 2 * i, R)).start()
            row_copy(out, buf, row, send, other, lax.rem(partner + 2 * i, R)).start()

        @pl.loop(far_both, half - 1)
        def _(j):
            i = chip_step(j)
            chip = lax.div(row, 2)
            row_copy(out, buf, row, send, same.at[chip], lax.rem(row + 2 * i, R)).start()

        row_copy(out, buf, row, send, other, partner).start()
        buf[pl.ds(pl.multiple_of(row * 8, 8), 8), :] = out[...]

    def row_finish(out, buf, send, same, other, far_both):
        @pl.loop(0, half - 1 - far_both)
        def _(j):
            slot = lax.rem(row + 2 * chip_step(half - 2 - j), R)
            row_copy(out, buf, slot, send, same.at[lax.div(slot, 2)], partner).wait_recv()
            row_copy(tile(buf, slot), buf, slot, send, other, partner).start()

        @pl.loop(0, far_both)
        def _(j):
            slot = lax.rem(row + 2 * chip_step(j), R)
            row_copy(out, buf, slot, send, same.at[lax.div(slot, 2)], partner).wait_recv()

        wait_tiles(buf, half, other)

    def col_copy(slot, peer):
        return pltpu.make_async_remote_copy(
            src_ref=out2,
            dst_ref=tile(buf2, slot),
            send_sem=s2,
            recv_sem=v2,
            device_id=(row, peer),
            device_id_type=MESH_ID,
        )

    loads["cn"].wait()
    loads["residual"].wait()
    half_way = mm(f["cn"], r_v)
    loads["cw"].wait()
    loads["pk"].wait()
    spec = mm(half_way, f["cw"], 1, 1)
    lams = f["pk"][16:24, :]
    p2 = f["pk"][0:8, :]
    p1 = f["pk"][24:32, :n]
    m8 = f["pk"][24:32, n:]
    columns = jnp.concatenate([lams[0:2, :n], p1[0:6]], axis=0).T
    weight = 1.0 / (columns[:, 1:2] + lams[0:1] + g)
    sol = weight * spec
    spec_v[...] = spec
    weight_v[...] = weight
    by_row = jnp.sum((sol * columns[:, 2:3]).reshape(n // 8, 8, w), axis=0)
    by_col = fold_lanes(sol * p2[0:1], min(w, 128))
    sign_row = 1.0 - 2.0 * (lax.broadcasted_iota(jnp.int32, (8, 1), 0) % 2).astype(jnp.float32)
    zf = jnp.sum(by_row, axis=0, keepdims=True)
    zl = jnp.sum(by_row * sign_row, axis=0, keepdims=True)
    signs_lane = 1.0 - 2.0 * (lax.broadcasted_iota(jnp.int32, (8, by_col.shape[1]), 1) % 2).astype(jnp.float32)
    odd_row = lax.broadcasted_iota(jnp.int32, (8, by_col.shape[1]), 0) % 2 == 1
    zb = mm(jnp.where(odd_row, signs_lane, 1.0), by_col, 1, 1)
    out1[...] = jnp.concatenate([zf[:, :n], zf[:, n:], zl[:, :n], zl[:, n:], zb[0:4]], axis=0)
    pl.semaphore_wait(barrier, half + C - 1 + far_most)
    row_start(out1, buf1, s1, v1, o1, far1)

    for name in rest:
        loads[name].wait()
    dev = f["dev"][...]
    base, far = chain(lams[0:1] + g, n)
    inv_v[...] = 1.0 / (base + far * f["s2"][...][:, 0:1])
    own_energy = fold_lanes(jnp.sum(spec_v[...] * spec_v[...] * weight_v[...], axis=0, keepdims=True), M)
    store3(w3, weight_v[...])
    store3(c3, f["cn"][...])
    store3(t3, f["tab"][...])
    row_finish(out1, buf1, s1, v1, o1, far1)
    y2 = mm(jnp.concatenate([f["qe"][...], dev[0:8, : 8 * R]], axis=0), buf1)
    mixed = y2[2 * R :]
    yl = jnp.concatenate([y2[:R], y2[R : 2 * R]], axis=1)
    yl_v[...] = yl
    tl = yl * inv_v[...]
    energy_r = fold_lanes(jnp.sum(yl * tl, axis=0, keepdims=True), M)
    q8 = jnp.dot(dev[8:16, : 6 * R].astype(jnp.bfloat16), tall6(tl), preferred_element_type=jnp.float32) * f["pk"][8:16, :]
    v8 = mm6(q8, w3, 1, 1) * m8
    z4 = jnp.concatenate(
        [
            mixed[0:1] + v8[0:1] + v8[2:3],
            mixed[1:2] + v8[4:5] + v8[6:7],
            mixed[2:3] + v8[1:2] + v8[3:4],
            mixed[3:4] + v8[5:6] + v8[7:8],
            jnp.zeros((4, n), jnp.float32),
        ],
        axis=0,
    )
    zp = mm6(z4, c3)
    re, im = zp[0:2], zp[2:4]
    rot = dev[24:32, :n]
    a1 = re * rot[0:1] + im * rot[1:2]
    b1 = re * rot[2:3] + im * rot[3:4]
    a2 = re * rot[4:5] + im * rot[5:6]
    b2 = re * rot[6:7] + im * rot[7:8]
    yy = mm6(jnp.concatenate([a1, a2, b1, b2], axis=0), t3)
    y4 = yy[0:4, :M] - yy[4:8, M:]
    zero3 = jnp.zeros((3, M), jnp.float32)
    out2[...] = jnp.concatenate([y4, own_energy - energy_r * (1.0 / R), zero3], axis=0)

    @pl.loop(1, C)
    def _(i):
        peer = lax.rem(col + i, C)
        col_copy(col, peer).start()

    buf2[pl.ds(pl.multiple_of(col * 8, 8), 8), :] = out2[...]

    base, far = chain(dev[5:6, : 2 * M] + g, w)
    norm = dev[6:7, : 2 * M]
    inv_c = norm / (base + far * f["s2"][...][:C, 1:2])
    cwh[...], cwl[...] = split(f["cw"][...])
    cth[...], ctl[...] = split(f["cn"][...].T)

    wait_tiles(buf2, C - 1, v2)

    y2 = mm(f["qc"], buf2)
    y = jnp.concatenate([y2[:C], y2[C : 2 * C]], axis=1)
    tl = y * inv_c
    energy = y2[2 * C : 2 * C + 1] - fold_lanes(jnp.sum(y * tl, axis=0, keepdims=True), M)
    q2 = jnp.dot(f["devc"][...][:, : 6 * C].astype(jnp.bfloat16), tall6(tl), preferred_element_type=jnp.float32)
    q4 = jnp.concatenate([q2[0:2, :M], q2[0:2, M:], jnp.zeros((4, M), jnp.float32)], axis=0)
    u = mm6(q4, [ref[:M, :M] for ref in t3], 1, 1)
    v = mm6(q4, [ref[:M, M:] for ref in t3], 1, 1)
    rot = rot[:, :M]
    re = u[0:2] * rot[0:1] - v[0:2] * rot[2:3] + u[2:4] * rot[4:5] - v[2:4] * rot[6:7]
    im = u[0:2] * rot[1:2] - v[0:2] * rot[3:4] + u[2:4] * rot[5:6] - v[2:4] * rot[7:8]
    out3[...] = jnp.concatenate([re, im, energy, zero3], axis=0)
    row_start(out3, buf3, s3, v3, o3, far3)
    wait_tiles(buf1, R - 1, s1)
    wait_tiles(buf2, C - 1, s2)
    row_finish(out3, buf3, s3, v3, o3, far3)

    xx = mm(jnp.concatenate([f["x3"][...], dev[16:24, : 8 * R]], axis=0), buf3)
    inner = jnp.sum(xx[4 * R + 2 : 4 * R + 3], axis=1, keepdims=True)
    xc = mm6(xx, [ref[:, :M] for ref in c3], 1, 1)
    moved = mm6(xc[: 2 * R] * m8[0:1] + xc[2 * R : 4 * R] * m8[2:3], w3)
    y_all = yl_v[...] + moved[:R] * p2[0:1] + moved[R:] * p2[1:2]
    row_flux = jnp.dot(dev[32:40, : 6 * R].astype(jnp.bfloat16), tall6(y_all * inv_v[...]), preferred_element_type=jnp.float32)
    sides = xc[4 * R : 4 * R + 4] * lams[2:3, :n] + xc[4 * R + 4 :] * lams[3:4, :n]
    left = jnp.concatenate([p1[0:4], sides], axis=0)
    right = jnp.concatenate([row_flux[0:4], p2[0:4]], axis=0)
    high, mid, low = split3(left)
    tall = jnp.concatenate([high, mid, low, high, mid, high], axis=0)
    low_rank = jnp.dot(tall.T.astype(jnp.bfloat16), tall6(right), preferred_element_type=jnp.float32)
    sol = weight_v[...] * (spec_v[...] + low_rank)
    wide = mm3(split(sol), (cwh, cwl))
    precond = mm3((cth, ctl), split(wide))
    next_ref[...] = precond
    inner_ref[...] = jnp.broadcast_to(inner, inner_ref.shape)
    wait_tiles(buf3, R - 1, s3)


def finish(scalar_ref, inner_ref, precond_ref, direction_ref, next_ref, ratio_ref):
    ratio = inner_ref[0:1, 0:1] / scalar_ref[1:2, 0:1]
    next_ref[...] = precond_ref[...] + ratio * direction_ref[...]
    ratio_ref[0] = jnp.sum(ratio)


def solution(mesh):
    R, C = mesh.shape["row"], mesh.shape["col"]

    def body(residual, direction, ground_shift, previous):
        n, w = residual.shape
        M = n // 2
        tables = make_tables(n, w, R, C)
        names = tuple(tables)
        shapes = [v.shape[1:] if k in ("dev", "devc") else v.shape for k, v in tables.items()]
        smem = pl.BlockSpec(memory_space=pltpu.SMEM)
        hbm = pl.BlockSpec(memory_space=pltpu.HBM)
        f32, bf16 = jnp.float32, jnp.bfloat16
        vm = lambda *shape: pltpu.VMEM(shape, f32)
        vb = lambda *shape: pltpu.VMEM(shape, bf16)
        dma = pltpu.SemaphoreType.DMA
        vmem = pl.BlockSpec(memory_space=pltpu.VMEM)
        held = lambda x: pltpu.with_memory_space_constraint(x, pltpu.HBM)
        lane = lax.broadcasted_iota(jnp.int32, (8, 128), 0)
        scalars = jnp.where(lane == 0, ground_shift, previous)
        precond, inner = pl.pallas_call(
            functools.partial(kernel, names, R, C),
            out_shape=(jax.ShapeDtypeStruct((n, w), f32), jax.ShapeDtypeStruct((8, 128), f32)),
            in_specs=[vmem] + [hbm] * (1 + len(names)),
            out_specs=(vmem, vmem),
            scratch_shapes=[pltpu.VMEM(s, f32) for s in shapes]
            + [vm(n, w), vm(8, n), vm(8, M), vm(8, M)]
            + [vm(8 * R, n), vm(8 * C, M), vm(8 * R, M)]
            + [vm(n, w), vm(n, w), vm(R, w), vm(R, w), vb(w, w), vb(w, w), vb(n, n), vb(n, n)]
            + [vb(n, w)] * 3 + [vb(n, n)] * 3 + [vb(n, n)] * 3
            + [dma((len(names) + 1,)), dma, dma((R // 2,)), dma, dma, dma, dma, dma((R // 2,)), dma],
            compiler_params=pltpu.CompilerParams(
                collective_id=0, has_side_effects=True, vmem_limit_bytes=24 * 2**20
            ),
        )(scalars, held(residual), *[held(jnp.asarray(v)) for v in tables.values()])
        return pl.pallas_call(
            finish,
            out_shape=(jax.ShapeDtypeStruct((n, w), f32), jax.ShapeDtypeStruct((1,), f32)),
            in_specs=[vmem] * 4,
            out_specs=(vmem, smem),
            compiler_params=pltpu.CompilerParams(vmem_limit_bytes=8 * 2**20),
        )(scalars, inner, precond, direction)

    return jax.shard_map(
        body,
        mesh=mesh,
        in_specs=(P("row", "col"), P("row", "col"), P(), P()),
        out_specs=(P("row", "col"), P()),
        check_vma=False,
    )
```

```python
import functools
import jax
import jax.numpy as jnp
import numpy as np
from jax import lax
from jax.experimental import pallas as pl
from jax.experimental.pallas import tpu as pltpu
from jax.sharding import PartitionSpec as P

HI = lax.Precision.HIGHEST
FAR1 = 0
FAR3 = 15


def mm(a, b, ca=1, cb=0):
    return lax.dot_general(
        a[...], b[...], (((ca,), (cb,)), ((), ())), precision=HI, preferred_element_type=jnp.float32
    )


def dct_table(n):
    k = np.arange(n)[:, None]
    p = np.arange(n)[None, :]
    table = np.sqrt(2.0 / n) * np.cos(np.pi * (k * (2 * p + 1) % (4 * n)) / (2 * n))
    table[0] = np.sqrt(1.0 / n)
    return table


def edge_sines(blocks):
    e = np.arange(1, blocks)
    q = np.zeros((blocks, blocks))
    q[: blocks - 1, : blocks - 1] = np.sqrt(2.0 / blocks) * np.sin(
        np.pi * (np.outer(e, e) % (2 * blocks)) / blocks
    )
    return q


def stack6(a):
    cut = lambda x: x.astype(np.float32).astype(jnp.bfloat16).astype(np.float64)
    high = cut(a)
    mid = cut(a - high)
    low = cut(a - high - mid)
    return np.concatenate([high, mid, low, high, mid, high], axis=-1)


def make_tables(n, w, R, C):
    assert w == 2 * n and R % 2 == 0 and C <= R
    M = n // 2
    f = {}
    cn, cw = dct_table(n), dct_table(w)
    even = np.where(np.arange(n) % 2 == 0, 1.0, 0.0)
    phi, sgn = cn[:, 0], 2 * even - 1
    phj, sgj = cw[:, 0], np.where(np.arange(w) % 2 == 0, 1.0, -1.0)
    f["cw"], f["cn"] = cw, cn
    pk = np.zeros((32, w))
    pk[0], pk[1] = phj, sgj * phj
    pk[8:12], pk[12:16] = phj, sgj * phj
    pk[16] = 4 * np.sin(np.pi * np.arange(w) / (2 * w)) ** 2
    pk[17, :n] = 4 * np.sin(np.pi * np.arange(n) / (2 * n)) ** 2
    pk[18, :n], pk[19, :n] = even, 1 - even
    pk[24, :n], pk[25, :n] = phi, sgn * phi
    for i in range(8):
        pk[24 + i, n:] = phi * (even if i in (0, 1, 4, 5) else 1 - even)
    f["pk"] = pk
    s2 = np.zeros((R, 128))
    s2[:, 0] = np.sin(np.pi * np.arange(1, R + 1) / (2 * R)) ** 2
    s2[:C, 1] = np.sin(np.pi * np.arange(1, C + 1) / (2 * C)) ** 2
    f["s2"] = s2

    t = np.arange(R)[:, None]
    d = np.arange(R)[None, :]
    ang = np.pi * (t * d % (2 * R)) / R
    mix_c, mix_s = np.cos(ang), np.sin(ang)
    mix_s[0] = np.where(np.arange(R) % 2 == 0, 1.0, -1.0)
    q_r, q_c = edge_sines(R), edge_sines(C)
    shift_r, shift_c = np.zeros((R, R)), np.zeros((C, C))
    shift_r[1:], shift_c[1:] = q_r[:-1], q_c[:-1]

    f["qe"] = np.zeros((R, max(256, 6 * R)))
    f["qe"][:, : 6 * R] = stack6(q_r.T)
    qc = np.zeros((2 * C + 8, C, 8))
    for a in range(2):
        qc[a * C : (a + 1) * C, :, 2 * a] = -shift_c.T
        qc[a * C : (a + 1) * C, :, 2 * a + 1] = q_c.T
    qc[2 * C, :, 4] = 1.0
    f["qc"] = qc.reshape(2 * C + 8, 8 * C)
    alt = np.where(np.arange(R) % 2 == 0, 1.0, -1.0)[:, None]
    fold = lambda mix, sign: mix + sign * alt * mix[:, ::-1]
    nxt = lambda m: np.concatenate([m[:, 1:], np.zeros((R, 1))], axis=1)
    x3 = np.zeros((2, 2, R, R, 8))
    for side in range(2):
        for part, mix in ((0, mix_c), (2, mix_s)):
            ev, od = fold(mix, 1.0), fold(mix, -1.0)
            x3[0, side, :, :, part + side] = q_r.T @ (ev - nxt(ev)).T
            x3[1, side, :, :, part + side] = -q_r.T @ (od + nxt(od)).T
    f["x3"] = x3.reshape(4 * R, 8 * R)

    p = np.arange(n)[:, None]
    m = np.arange(M)[None, :]
    a_ang = np.pi * (m * (2 * p + 1) % (2 * n)) / n
    f["tab"] = np.concatenate([np.cos(a_ang), np.sin(a_ang)], axis=1)

    lanes = max(8 * R, n, 2 * M, 256)
    dev = np.zeros((R, 40, lanes))
    pos = 2 * np.arange(n) + 1
    N = n * R
    for r in range(R):
        nz = float(r > 0)
        dev[r, 0, : 6 * R] = stack6(mix_c[r])
        dev[r, 1, : 6 * R] = stack6(mix_s[r])
        for part, mix in ((0, mix_c), (1, mix_s)):
            top = mix[r] @ shift_r
            bot = -(mix[r] @ q_r)
            dev[r, 8 + part, : 6 * R] = stack6(top + bot)
            dev[r, 10 + part, : 6 * R] = stack6(top - bot)
        dev[r, 32, : 6 * R] = stack6(shift_r[r])
        dev[r, 33, : 6 * R] = stack6(-q_r[r])
        for base, sign in ((16, 1.0), (20, -1.0)):
            for side in range(2):
                row = np.zeros((R, 8))
                row[:, side] = fold(mix_c, sign)[:, r]
                row[:, 2 + side] = fold(mix_s, sign)[:, r]
                dev[r, base + side, : 8 * R] = row.reshape(-1)
        row = np.zeros((R, 8))
        row[:, 4] = 1.0
        dev[r, 18, : 8 * R] = row.reshape(-1)
        tau = (r, 2 * R - r if r > 0 else R)
        ca, sa = [], []
        for x in tau:
            b = np.pi * (x * pos % (4 * N)) / (2 * N)
            ca.append(np.cos(b))
            sa.append(np.sin(b))
        rot = [ca[0], -nz * sa[0], sa[0], nz * ca[0]]
        if r > 0:
            rot += [ca[1], sa[1], sa[1], -ca[1]]
        else:
            rot += [0 * pos, ca[1], 0 * pos, sa[1]]
        for i, v in enumerate(rot):
            dev[r, 24 + i, :n] = v
        k = np.concatenate([2 * R * np.arange(M) + x for x in tau])
        dev[r, 34, : 2 * M] = 4 * np.sin(np.pi * k / (2 * N)) ** 2
        dev[r, 35, : 2 * M] = np.where(k == 0, 1.0 / N, 2.0 / N)
    f["dev"] = dev
    devc = np.zeros((C, 8, 128))
    for c in range(C):
        devc[c, 0, : 6 * C] = stack6(shift_c[c])
        devc[c, 1, : 6 * C] = stack6(-q_c[c])
    f["devc"] = devc
    return {key: v.astype(np.float32) for key, v in f.items()}


def chain(mu, n):
    s = 0.5 * jnp.sqrt(mu)
    ch = jnp.sqrt(1.0 + s * s)
    x = s + s * s / (1.0 + ch)
    z = x / (2.0 + x)
    z2 = z * z
    acc = jnp.full_like(z, 1.0 / 19.0)
    for k in (17, 15, 13, 11, 9, 7, 5, 3, 1):
        acc = acc * z2 + 1.0 / k
    theta = 4.0 * z * acc
    decay = jnp.exp(-n * theta)
    shorter = jnp.exp(-(n - 1) * theta)
    diff = (ch - s) * (1.0 - shorter) / (2.0 * s * (1.0 + decay))
    far = ch * decay / (s * (1.0 - decay * decay))
    return 1.0 + 2.0 * diff, 4.0 * far


def split(x):
    high = x.astype(jnp.bfloat16)
    return high, (x - high.astype(jnp.float32)).astype(jnp.bfloat16)


def mm3(a, b):
    dot = lambda x, y: jnp.dot(x[...], y[...], preferred_element_type=jnp.float32)
    return dot(a[0], b[0]) + (dot(a[0], b[1]) + dot(a[1], b[0]))


def split3(x):
    high = x.astype(jnp.bfloat16).astype(jnp.float32)
    rest = x - high
    mid = rest.astype(jnp.bfloat16).astype(jnp.float32)
    return high, mid, rest - mid


def store3(refs, x):
    for ref, part in zip(refs, split3(x)):
        ref[...] = part.astype(jnp.bfloat16)


def mm6(a, b, ca=1, cb=0):
    rows = a.shape[0]
    a3 = jnp.concatenate(split3(a), axis=0).astype(jnp.bfloat16)
    dot = lambda x, y: lax.dot_general(
        x, y[...], (((ca,), (cb,)), ((), ())), preferred_element_type=jnp.float32
    )
    p0, p1, p2 = dot(a3, b[0]), dot(a3[: 2 * rows], b[1]), dot(a3[: 2 * rows], b[2])
    low = p0[2 * rows :] + p1[rows:] + p2[:rows]
    return p0[:rows] + (p0[rows : 2 * rows] + p1[:rows] + low)


def full_tiles(buf):
    x = buf[...]
    slots, rows, lanes = x.shape
    padded = -(-rows // 8) * 8
    rest = jnp.zeros((slots, padded - rows, lanes), jnp.float32)
    return jnp.concatenate([x, rest], axis=1).reshape(padded * slots, lanes)


def tall6(b):
    high, mid, low = split3(b)
    return jnp.concatenate([high, high, high, mid, mid, low], axis=0).astype(jnp.bfloat16)


def fold_lanes(x, width):
    out = x[:, :width]
    for i in range(1, x.shape[1] // width):
        out = out + x[:, i * width : (i + 1) * width]
    return out


MESH_ID = pl.DeviceIdType.MESH


def kernel(names, R, C, *refs):
    count = len(names)
    scalar_ref, residual_ref = refs[:2]
    table_hbm = refs[2 : 2 + count]
    next_ref, inner_ref = refs[2 + count : 4 + count]
    refs = refs[4 + count :]
    table_v, refs = refs[:count], refs[count:]
    (r_v, out1, out2, out3, buf1, buf2, buf3), refs = refs[:7], refs[7:]
    (spec_v, weight_v, yl_v, inv_v, cwh, cwl, cth, ctl), refs = refs[:8], refs[8:]
    w3, c3, t3, refs = refs[:3], refs[3:6], refs[6:9], refs[9:]
    load_sem, s1, v1, o1, s2, v2, s3, v3, o3 = refs
    row, col = lax.axis_index("row"), lax.axis_index("col")
    half = R // 2
    partner = row + 1 - 2 * lax.rem(row, 2)
    n, w = r_v.shape
    M = n // 2
    far1, far3 = min(FAR1, half - 1), min(FAR3, half - 1)
    far_most = max(far1, far3)

    def chip_step(j):
        return half // 2 + lax.div(j + 1, 2) * (1 - 2 * lax.rem(j, 2))


    loads = {}
    for i, name in enumerate(names):
        src = table_hbm[i]
        if name == "dev":
            src = src.at[row]
        elif name == "devc":
            src = src.at[col]
        loads[name] = pltpu.make_async_copy(src, table_v[i], load_sem.at[i])
    loads["residual"] = pltpu.make_async_copy(residual_ref, r_v, load_sem.at[count])
    first = ("cn", "residual", "cw", "pk")
    rest = tuple(x for x in names if x not in first)
    for name in first:
        loads[name].start()

    barrier = pltpu.get_barrier_semaphore()

    @pl.loop(1, half)
    def _(i):
        peer = lax.rem(row + 2 * i, R)
        pl.semaphore_signal(barrier, inc=1, device_id=(peer, col), device_id_type=MESH_ID)

    @pl.loop(1, C)
    def _(i):
        peer = lax.rem(col + i, C)
        pl.semaphore_signal(barrier, inc=1, device_id=(row, peer), device_id_type=MESH_ID)

    @pl.loop(0, far_most)
    def _(j):
        peer = lax.rem(partner + 2 * chip_step(j), R)
        pl.semaphore_signal(barrier, inc=1, device_id=(peer, col), device_id_type=MESH_ID)

    pl.semaphore_signal(barrier, inc=1, device_id=(partner, col), device_id_type=MESH_ID)

    for name in rest:
        loads[name].start()
    f = dict(zip(names, table_v))
    g = scalar_ref[0:1, 0:1]

    def tile(buf, slot):
        return buf.at[slot]

    def row_copy(src, buf, slot, send, recv, peer):
        return pltpu.make_async_remote_copy(
            src_ref=src,
            dst_ref=tile(buf, slot),
            send_sem=send,
            recv_sem=recv,
            device_id=(peer, col),
            device_id_type=MESH_ID,
        )

    def wait_tiles(buf, tiles, sem):
        part = buf.at[pl.ds(0, tiles)]
        pltpu.make_async_copy(part, part, sem).wait()

    def row_start(out, buf, send, same, other, far_both):
        @pl.loop(0, far_both)
        def _(j):
            i = chip_step(j)
            chip = lax.div(row, 2)
            row_copy(out, buf, row, send, same.at[chip], lax.rem(row + 2 * i, R)).start()
            row_copy(out, buf, row, send, other, lax.rem(partner + 2 * i, R)).start()

        @pl.loop(far_both, half - 1)
        def _(j):
            i = chip_step(j)
            chip = lax.div(row, 2)
            row_copy(out, buf, row, send, same.at[chip], lax.rem(row + 2 * i, R)).start()

        row_copy(out, buf, row, send, other, partner).start()
        buf[row] = out[...]

    def row_finish(out, buf, send, same, other, far_both):
        @pl.loop(0, half - 1 - far_both)
        def _(j):
            slot = lax.rem(row + 2 * chip_step(half - 2 - j), R)
            row_copy(out, buf, slot, send, same.at[lax.div(slot, 2)], partner).wait_recv()
            row_copy(tile(buf, slot), buf, slot, send, other, partner).start()

        @pl.loop(0, far_both)
        def _(j):
            slot = lax.rem(row + 2 * chip_step(j), R)
            row_copy(out, buf, slot, send, same.at[lax.div(slot, 2)], partner).wait_recv()

        wait_tiles(buf, half, other)

    def col_copy(slot, peer):
        return pltpu.make_async_remote_copy(
            src_ref=out2,
            dst_ref=tile(buf2, slot),
            send_sem=s2,
            recv_sem=v2,
            device_id=(row, peer),
            device_id_type=MESH_ID,
        )

    loads["cn"].wait()
    loads["residual"].wait()
    half_way = mm(f["cn"], r_v)
    loads["cw"].wait()
    loads["pk"].wait()
    spec = mm(half_way, f["cw"], 1, 1)
    lams = f["pk"][16:24, :]
    p2 = f["pk"][0:8, :]
    p1 = f["pk"][24:32, :n]
    m8 = f["pk"][24:32, n:]
    columns = jnp.concatenate([lams[0:2, :n], p1[0:6]], axis=0).T
    weight = 1.0 / (columns[:, 1:2] + lams[0:1] + g)
    sol = weight * spec
    spec_v[...] = spec
    weight_v[...] = weight
    by_row = jnp.sum((sol * columns[:, 2:3]).reshape(n // 8, 8, w), axis=0)
    by_col = fold_lanes(sol * p2[0:1], min(w, 128))
    sign_row = 1.0 - 2.0 * (lax.broadcasted_iota(jnp.int32, (8, 1), 0) % 2).astype(jnp.float32)
    zf = jnp.sum(by_row, axis=0, keepdims=True)
    zl = jnp.sum(by_row * sign_row, axis=0, keepdims=True)
    signs_lane = 1.0 - 2.0 * (lax.broadcasted_iota(jnp.int32, (8, by_col.shape[1]), 1) % 2).astype(jnp.float32)
    odd_row = lax.broadcasted_iota(jnp.int32, (8, by_col.shape[1]), 0) % 2 == 1
    zb = mm(jnp.where(odd_row, signs_lane, 1.0), by_col, 1, 1)
    cut = lambda x: [x[:, i * M : (i + 1) * M] for i in range(x.shape[1] // M)]
    out1[...] = jnp.concatenate(cut(zf) + cut(zl) + cut(zb[0:1]) + cut(zb[1:2]), axis=0)
    pl.semaphore_wait(barrier, half + C - 1 + far_most)
    row_start(out1, buf1, s1, v1, o1, far1)

    for name in rest:
        loads[name].wait()
    dev = f["dev"][...]
    base, far = chain(lams[0:1] + g, n)
    inv_v[...] = 1.0 / (base + far * f["s2"][...][:, 0:1])
    own_energy = fold_lanes(jnp.sum(spec_v[...] * spec_v[...] * weight_v[...], axis=0, keepdims=True), M)
    store3(w3, weight_v[...])
    store3(c3, f["cn"][...])
    store3(t3, f["tab"][...])
    row_finish(out1, buf1, s1, v1, o1, far1)
    wide_rows = lambda first, count: jnp.concatenate(
        [buf1[:, first + k, :] for k in range(count)], axis=1
    )
    last, head = wide_rows(4, 4), wide_rows(0, 4)
    jump = last - jnp.concatenate([head[1:], head[:1]], axis=0)
    yl = jnp.dot(f["qe"][:, : 6 * R].astype(jnp.bfloat16), tall6(jump), preferred_element_type=jnp.float32)
    mixed = jnp.dot(dev[0:8, : 6 * R].astype(jnp.bfloat16), tall6(wide_rows(8, 4)), preferred_element_type=jnp.float32)
    yl_v[...] = yl
    tl = yl * inv_v[...]
    energy_r = fold_lanes(jnp.sum(yl * tl, axis=0, keepdims=True), M)
    q8 = jnp.dot(dev[8:16, : 6 * R].astype(jnp.bfloat16), tall6(tl), preferred_element_type=jnp.float32)
    q8 = jnp.concatenate([q8[0:4], q8[0:4]], axis=0) * f["pk"][8:16, :]
    v8 = mm6(q8, w3, 1, 1) * m8
    z4 = jnp.concatenate(
        [
            mixed[0:1, :n] + v8[0:1] + v8[2:3],
            mixed[0:1, n:] + v8[4:5] + v8[6:7],
            mixed[1:2, :n] + v8[1:2] + v8[3:4],
            mixed[1:2, n:] + v8[5:6] + v8[7:8],
            jnp.zeros((4, n), jnp.float32),
        ],
        axis=0,
    )
    zp = mm6(z4, c3)
    re, im = zp[0:2], zp[2:4]
    rot = dev[24:32, :n]
    a1 = re * rot[0:1] + im * rot[1:2]
    b1 = re * rot[2:3] + im * rot[3:4]
    a2 = re * rot[4:5] + im * rot[5:6]
    b2 = re * rot[6:7] + im * rot[7:8]
    yy = mm6(jnp.concatenate([a1, a2, b1, b2], axis=0), t3)
    y4 = yy[0:4, :M] - yy[4:8, M:]
    out2[...] = jnp.concatenate([y4, own_energy - energy_r * (1.0 / R)], axis=0)

    @pl.loop(1, C)
    def _(i):
        peer = lax.rem(col + i, C)
        col_copy(col, peer).start()

    buf2[col] = out2[...]

    base, far = chain(dev[34:35, : 2 * M] + g, w)
    norm = dev[35:36, : 2 * M]
    inv_c = norm / (base + far * f["s2"][...][:C, 1:2])
    cwh[...], cwl[...] = split(f["cw"][...])
    cth[...], ctl[...] = split(f["cn"][...].T)

    wait_tiles(buf2, C - 1, v2)

    y2 = mm(f["qc"], full_tiles(buf2))
    y = jnp.concatenate([y2[:C], y2[C : 2 * C]], axis=1)
    tl = y * inv_c
    energy = y2[2 * C : 2 * C + 1] - fold_lanes(jnp.sum(y * tl, axis=0, keepdims=True), M)
    q2 = jnp.dot(f["devc"][...][:, : 6 * C].astype(jnp.bfloat16), tall6(tl), preferred_element_type=jnp.float32)
    q4 = jnp.concatenate([q2[0:2, :M], q2[0:2, M:], jnp.zeros((4, M), jnp.float32)], axis=0)
    u = mm6(q4, [ref[:M, :M] for ref in t3], 1, 1)
    v = mm6(q4, [ref[:M, M:] for ref in t3], 1, 1)
    rot = rot[:, :M]
    re = u[0:2] * rot[0:1] - v[0:2] * rot[2:3] + u[2:4] * rot[4:5] - v[2:4] * rot[6:7]
    im = u[0:2] * rot[1:2] - v[0:2] * rot[3:4] + u[2:4] * rot[5:6] - v[2:4] * rot[7:8]
    out3[...] = jnp.concatenate([re, im, energy], axis=0)
    row_start(out3, buf3, s3, v3, o3, far3)
    wait_tiles(buf1, R - 1, s1)
    wait_tiles(buf2, C - 1, s2)
    row_finish(out3, buf3, s3, v3, o3, far3)

    xx = mm(jnp.concatenate([f["x3"][...], dev[16:24, : 8 * R]], axis=0), full_tiles(buf3))
    inner = jnp.sum(xx[4 * R + 2 : 4 * R + 3], axis=1, keepdims=True)
    xc = mm6(xx, [ref[:, :M] for ref in c3], 1, 1)
    moved = mm6(xc[: 2 * R] * m8[0:1] + xc[2 * R : 4 * R] * m8[2:3], w3)
    y_all = yl_v[...] + moved[:R] * p2[0:1] + moved[R:] * p2[1:2]
    row_flux = jnp.dot(dev[32:40, : 6 * R].astype(jnp.bfloat16), tall6(y_all * inv_v[...]), preferred_element_type=jnp.float32)
    sides = xc[4 * R : 4 * R + 4] * lams[2:3, :n] + xc[4 * R + 4 :] * lams[3:4, :n]
    left = jnp.concatenate([p1[0:4], sides], axis=0)
    right = jnp.concatenate([row_flux[0:4], p2[0:4]], axis=0)
    high, mid, low = split3(left)
    tall = jnp.concatenate([high, mid, low, high, mid, high], axis=0)
    low_rank = jnp.dot(tall.T.astype(jnp.bfloat16), tall6(right), preferred_element_type=jnp.float32)
    sol = weight_v[...] * (spec_v[...] + low_rank)
    wide = mm3(split(sol), (cwh, cwl))
    precond = mm3((cth, ctl), split(wide))
    next_ref[...] = precond
    inner_ref[...] = jnp.broadcast_to(inner, inner_ref.shape)
    wait_tiles(buf3, R - 1, s3)


def finish(scalar_ref, inner_ref, precond_ref, direction_ref, next_ref, ratio_ref):
    ratio = inner_ref[0:1, 0:1] / scalar_ref[1:2, 0:1]
    next_ref[...] = precond_ref[...] + ratio * direction_ref[...]
    ratio_ref[0] = jnp.sum(ratio)


def solution(mesh):
    R, C = mesh.shape["row"], mesh.shape["col"]

    def body(residual, direction, ground_shift, previous):
        n, w = residual.shape
        M = n // 2
        tables = make_tables(n, w, R, C)
        names = tuple(tables)
        shapes = [v.shape[1:] if k in ("dev", "devc") else v.shape for k, v in tables.items()]
        smem = pl.BlockSpec(memory_space=pltpu.SMEM)
        hbm = pl.BlockSpec(memory_space=pltpu.HBM)
        f32, bf16 = jnp.float32, jnp.bfloat16
        vm = lambda *shape: pltpu.VMEM(shape, f32)
        vb = lambda *shape: pltpu.VMEM(shape, bf16)
        dma = pltpu.SemaphoreType.DMA
        vmem = pl.BlockSpec(memory_space=pltpu.VMEM)
        held = lambda x: pltpu.with_memory_space_constraint(x, pltpu.HBM)
        lane = lax.broadcasted_iota(jnp.int32, (8, 128), 0)
        scalars = jnp.where(lane == 0, ground_shift, previous)
        precond, inner = pl.pallas_call(
            functools.partial(kernel, names, R, C),
            out_shape=(jax.ShapeDtypeStruct((n, w), f32), jax.ShapeDtypeStruct((8, 128), f32)),
            in_specs=[vmem] + [hbm] * (1 + len(names)),
            out_specs=(vmem, vmem),
            scratch_shapes=[pltpu.VMEM(s, f32) for s in shapes]
            + [vm(n, w), vm(12, M), vm(5, M), vm(5, M)]
            + [vm(R, 12, M), vm(C, 5, M), vm(R, 5, M)]
            + [vm(n, w), vm(n, w), vm(R, w), vm(R, w), vb(w, w), vb(w, w), vb(n, n), vb(n, n)]
            + [vb(n, w)] * 3 + [vb(n, n)] * 3 + [vb(n, n)] * 3
            + [dma((len(names) + 1,)), dma, dma((R // 2,)), dma, dma, dma, dma, dma((R // 2,)), dma],
            compiler_params=pltpu.CompilerParams(
                collective_id=0, has_side_effects=True, vmem_limit_bytes=24 * 2**20
            ),
        )(scalars, held(residual), *[held(jnp.asarray(v)) for v in tables.values()])
        return pl.pallas_call(
            finish,
            out_shape=(jax.ShapeDtypeStruct((n, w), f32), jax.ShapeDtypeStruct((1,), f32)),
            in_specs=[vmem] * 4,
            out_specs=(vmem, smem),
            compiler_params=pltpu.CompilerParams(vmem_limit_bytes=8 * 2**20),
        )(scalars, inner, precond, direction)

    return jax.shard_map(
        body,
        mesh=mesh,
        in_specs=(P("row", "col"), P("row", "col"), P(), P()),
        out_specs=(P("row", "col"), P()),
        check_vma=False,
    )
```

```python
import functools
import jax
import jax.numpy as jnp
import numpy as np
from jax import lax
from jax.experimental import pallas as pl
from jax.experimental.pallas import tpu as pltpu
from jax.sharding import PartitionSpec as P

HI = lax.Precision.HIGHEST
FAR1 = 0
FAR3 = 15


def mm(a, b, ca=1, cb=0):
    return lax.dot_general(
        a[...], b[...], (((ca,), (cb,)), ((), ())), precision=HI, preferred_element_type=jnp.float32
    )


def dct_table(n):
    k = np.arange(n)[:, None]
    p = np.arange(n)[None, :]
    table = np.sqrt(2.0 / n) * np.cos(np.pi * (k * (2 * p + 1) % (4 * n)) / (2 * n))
    table[0] = np.sqrt(1.0 / n)
    return table


def edge_sines(blocks):
    e = np.arange(1, blocks)
    q = np.zeros((blocks, blocks))
    q[: blocks - 1, : blocks - 1] = np.sqrt(2.0 / blocks) * np.sin(
        np.pi * (np.outer(e, e) % (2 * blocks)) / blocks
    )
    return q


def stack6(a):
    cut = lambda x: x.astype(np.float32).astype(jnp.bfloat16).astype(np.float64)
    high = cut(a)
    mid = cut(a - high)
    low = cut(a - high - mid)
    return np.concatenate([high, mid, low, high, mid, high], axis=-1)


def make_tables(n, w, R, C):
    assert w == 2 * n and R % 2 == 0 and C <= R
    M = n // 2
    f = {}
    cn, cw = dct_table(n), dct_table(w)
    even = np.where(np.arange(n) % 2 == 0, 1.0, 0.0)
    phi, sgn = cn[:, 0], 2 * even - 1
    phj, sgj = cw[:, 0], np.where(np.arange(w) % 2 == 0, 1.0, -1.0)
    f["cw"], f["cn"] = cw, cn
    pk = np.zeros((32, w))
    pk[0], pk[1] = phj, sgj * phj
    pk[8:12], pk[12:16] = phj, sgj * phj
    pk[16] = 4 * np.sin(np.pi * np.arange(w) / (2 * w)) ** 2
    pk[17, :n] = 4 * np.sin(np.pi * np.arange(n) / (2 * n)) ** 2
    pk[18, :n], pk[19, :n] = even, 1 - even
    pk[24, :n], pk[25, :n] = phi, sgn * phi
    for i in range(8):
        pk[24 + i, n:] = phi * (even if i in (0, 1, 4, 5) else 1 - even)
    f["pk"] = pk
    s2 = np.zeros((R, 128))
    s2[:, 0] = np.sin(np.pi * np.arange(1, R + 1) / (2 * R)) ** 2
    s2[:C, 1] = np.sin(np.pi * np.arange(1, C + 1) / (2 * C)) ** 2
    f["s2"] = s2

    t = np.arange(R)[:, None]
    d = np.arange(R)[None, :]
    ang = np.pi * (t * d % (2 * R)) / R
    mix_c, mix_s = np.cos(ang), np.sin(ang)
    mix_s[0] = np.where(np.arange(R) % 2 == 0, 1.0, -1.0)
    q_r, q_c = edge_sines(R), edge_sines(C)
    shift_r, shift_c = np.zeros((R, R)), np.zeros((C, C))
    shift_r[1:], shift_c[1:] = q_r[:-1], q_c[:-1]

    f["qe"] = np.zeros((R, max(256, 6 * R)))
    f["qe"][:, : 6 * R] = stack6(q_r.T)
    f["qc"] = np.zeros((C, max(128, 6 * C)))
    f["qc"][:, : 6 * C] = stack6(q_c.T)
    alt = np.where(np.arange(R) % 2 == 0, 1.0, -1.0)[:, None]
    fold = lambda mix, sign: mix + sign * alt * mix[:, ::-1]
    nxt = lambda m: np.concatenate([m[:, 1:], np.zeros((R, 1))], axis=1)
    x3 = np.zeros((2, R, 2 * R))
    for part, mix in ((0, mix_c), (R, mix_s)):
        ev, od = fold(mix, 1.0), fold(mix, -1.0)
        x3[0, :, part : part + R] = q_r.T @ (ev - nxt(ev)).T
        x3[1, :, part : part + R] = -q_r.T @ (od + nxt(od)).T
    f["x3"] = stack6(x3.reshape(2 * R, 2 * R))

    p = np.arange(n)[:, None]
    m = np.arange(M)[None, :]
    a_ang = np.pi * (m * (2 * p + 1) % (2 * n)) / n
    f["tab"] = np.concatenate([np.cos(a_ang), np.sin(a_ang)], axis=1)

    lanes = max(8 * R, n, 2 * M, 256)
    dev = np.zeros((R, 48, lanes))
    pos = 2 * np.arange(n) + 1
    N = n * R
    for r in range(R):
        nz = float(r > 0)
        dev[r, 0, : 6 * R] = stack6(mix_c[r])
        dev[r, 1, : 6 * R] = stack6(mix_s[r])
        for part, mix in ((0, mix_c), (1, mix_s)):
            top = mix[r] @ shift_r
            bot = -(mix[r] @ q_r)
            dev[r, 8 + part, : 6 * R] = stack6(top + bot)
            dev[r, 10 + part, : 6 * R] = stack6(top - bot)
        dev[r, 32, : 6 * R] = stack6(shift_r[r])
        dev[r, 33, : 6 * R] = stack6(-q_r[r])
        for base, sign in ((0, 1.0), (1, -1.0)):
            both = np.concatenate([fold(mix_c, sign)[:, r], fold(mix_s, sign)[:, r]])
            first, second = np.split(stack6(both), [8 * R])
            dev[r, 16 + base, : 8 * R] = first
            dev[r, 40 + base, : 4 * R] = second
        tau = (r, 2 * R - r if r > 0 else R)
        ca, sa = [], []
        for x in tau:
            b = np.pi * (x * pos % (4 * N)) / (2 * N)
            ca.append(np.cos(b))
            sa.append(np.sin(b))
        rot = [ca[0], -nz * sa[0], sa[0], nz * ca[0]]
        if r > 0:
            rot += [ca[1], sa[1], sa[1], -ca[1]]
        else:
            rot += [0 * pos, ca[1], 0 * pos, sa[1]]
        for i, v in enumerate(rot):
            dev[r, 24 + i, :n] = v
        k = np.concatenate([2 * R * np.arange(M) + x for x in tau])
        dev[r, 34, : 2 * M] = 4 * np.sin(np.pi * k / (2 * N)) ** 2
        dev[r, 35, : 2 * M] = np.where(k == 0, 1.0 / N, 2.0 / N)
    f["dev"] = dev
    devc = np.zeros((C, 8, 128))
    for c in range(C):
        devc[c, 0, : 6 * C] = stack6(shift_c[c])
        devc[c, 1, : 6 * C] = stack6(-q_c[c])
    f["devc"] = devc
    return {key: v.astype(np.float32) for key, v in f.items()}


def chain(mu, n):
    s = 0.5 * jnp.sqrt(mu)
    ch = jnp.sqrt(1.0 + s * s)
    x = s + s * s / (1.0 + ch)
    z = x / (2.0 + x)
    z2 = z * z
    acc = jnp.full_like(z, 1.0 / 19.0)
    for k in (17, 15, 13, 11, 9, 7, 5, 3, 1):
        acc = acc * z2 + 1.0 / k
    theta = 4.0 * z * acc
    decay = jnp.exp(-n * theta)
    shorter = jnp.exp(-(n - 1) * theta)
    diff = (ch - s) * (1.0 - shorter) / (2.0 * s * (1.0 + decay))
    far = ch * decay / (s * (1.0 - decay * decay))
    return 1.0 + 2.0 * diff, 4.0 * far


def split(x):
    high = x.astype(jnp.bfloat16)
    return high, (x - high.astype(jnp.float32)).astype(jnp.bfloat16)


def mm3(a, b):
    dot = lambda x, y: jnp.dot(x[...], y[...], preferred_element_type=jnp.float32)
    return dot(a[0], b[0]) + (dot(a[0], b[1]) + dot(a[1], b[0]))


def split3(x):
    high = x.astype(jnp.bfloat16).astype(jnp.float32)
    rest = x - high
    mid = rest.astype(jnp.bfloat16).astype(jnp.float32)
    return high, mid, rest - mid


def store3(refs, x):
    for ref, part in zip(refs, split3(x)):
        ref[...] = part.astype(jnp.bfloat16)


def mm6(a, b, ca=1, cb=0):
    rows = a.shape[0]
    a3 = jnp.concatenate(split3(a), axis=0).astype(jnp.bfloat16)
    dot = lambda x, y: lax.dot_general(
        x, y[...], (((ca,), (cb,)), ((), ())), preferred_element_type=jnp.float32
    )
    p0, p1, p2 = dot(a3, b[0]), dot(a3[: 2 * rows], b[1]), dot(a3[: 2 * rows], b[2])
    low = p0[2 * rows :] + p1[rows:] + p2[:rows]
    return p0[:rows] + (p0[rows : 2 * rows] + p1[:rows] + low)


def tall6(b):
    high, mid, low = split3(b)
    return jnp.concatenate([high, high, high, mid, mid, low], axis=0).astype(jnp.bfloat16)


def fold_lanes(x, width):
    out = x[:, :width]
    for i in range(1, x.shape[1] // width):
        out = out + x[:, i * width : (i + 1) * width]
    return out


MESH_ID = pl.DeviceIdType.MESH


def kernel(names, R, C, *refs):
    count = len(names)
    scalar_ref, residual_ref = refs[:2]
    table_hbm = refs[2 : 2 + count]
    next_ref, inner_ref = refs[2 + count : 4 + count]
    refs = refs[4 + count :]
    table_v, refs = refs[:count], refs[count:]
    (r_v, out1, out2, out3, buf1, buf2, buf3), refs = refs[:7], refs[7:]
    (spec_v, weight_v, yl_v, inv_v, cwh, cwl, cth, ctl), refs = refs[:8], refs[8:]
    w3, c3, t3, refs = refs[:3], refs[3:6], refs[6:9], refs[9:]
    load_sem, s1, v1, o1, s2, v2, s3, v3, o3 = refs
    row, col = lax.axis_index("row"), lax.axis_index("col")
    half = R // 2
    partner = row + 1 - 2 * lax.rem(row, 2)
    n, w = r_v.shape
    M = n // 2
    far1, far3 = min(FAR1, half - 1), min(FAR3, half - 1)
    far_most = max(far1, far3)

    def chip_step(j):
        return half // 2 + lax.div(j + 1, 2) * (1 - 2 * lax.rem(j, 2))


    loads = {}
    for i, name in enumerate(names):
        src = table_hbm[i]
        if name == "dev":
            src = src.at[row]
        elif name == "devc":
            src = src.at[col]
        loads[name] = pltpu.make_async_copy(src, table_v[i], load_sem.at[i])
    loads["residual"] = pltpu.make_async_copy(residual_ref, r_v, load_sem.at[count])
    first = ("cn", "residual", "cw", "pk")
    rest = tuple(x for x in names if x not in first)
    for name in first:
        loads[name].start()

    barrier = pltpu.get_barrier_semaphore()

    @pl.loop(1, half)
    def _(i):
        peer = lax.rem(row + 2 * i, R)
        pl.semaphore_signal(barrier, inc=1, device_id=(peer, col), device_id_type=MESH_ID)

    @pl.loop(1, C)
    def _(i):
        peer = lax.rem(col + i, C)
        pl.semaphore_signal(barrier, inc=1, device_id=(row, peer), device_id_type=MESH_ID)

    @pl.loop(0, far_most)
    def _(j):
        peer = lax.rem(partner + 2 * chip_step(j), R)
        pl.semaphore_signal(barrier, inc=1, device_id=(peer, col), device_id_type=MESH_ID)

    pl.semaphore_signal(barrier, inc=1, device_id=(partner, col), device_id_type=MESH_ID)

    for name in rest:
        loads[name].start()
    f = dict(zip(names, table_v))
    g = scalar_ref[0:1, 0:1]

    def tile(buf, slot):
        return buf.at[slot]

    def row_copy(src, buf, slot, send, recv, peer):
        return pltpu.make_async_remote_copy(
            src_ref=src,
            dst_ref=tile(buf, slot),
            send_sem=send,
            recv_sem=recv,
            device_id=(peer, col),
            device_id_type=MESH_ID,
        )

    def wait_tiles(buf, tiles, sem):
        part = buf.at[pl.ds(0, tiles)]
        pltpu.make_async_copy(part, part, sem).wait()

    def row_start(out, buf, send, same, other, far_both):
        @pl.loop(0, far_both)
        def _(j):
            i = chip_step(j)
            chip = lax.div(row, 2)
            row_copy(out, buf, row, send, same.at[chip], lax.rem(row + 2 * i, R)).start()
            row_copy(out, buf, row, send, other, lax.rem(partner + 2 * i, R)).start()

        @pl.loop(far_both, half - 1)
        def _(j):
            i = chip_step(j)
            chip = lax.div(row, 2)
            row_copy(out, buf, row, send, same.at[chip], lax.rem(row + 2 * i, R)).start()

        row_copy(out, buf, row, send, other, partner).start()
        buf[row] = out[...]

    def row_finish(out, buf, send, same, other, far_both):
        @pl.loop(0, half - 1 - far_both)
        def _(j):
            slot = lax.rem(row + 2 * chip_step(half - 2 - j), R)
            row_copy(out, buf, slot, send, same.at[lax.div(slot, 2)], partner).wait_recv()
            row_copy(tile(buf, slot), buf, slot, send, other, partner).start()

        @pl.loop(0, far_both)
        def _(j):
            slot = lax.rem(row + 2 * chip_step(j), R)
            row_copy(out, buf, slot, send, same.at[lax.div(slot, 2)], partner).wait_recv()

        wait_tiles(buf, half, other)

    def col_copy(slot, peer):
        return pltpu.make_async_remote_copy(
            src_ref=out2,
            dst_ref=tile(buf2, slot),
            send_sem=s2,
            recv_sem=v2,
            device_id=(row, peer),
            device_id_type=MESH_ID,
        )

    loads["cn"].wait()
    loads["residual"].wait()
    half_way = mm(f["cn"], r_v)
    loads["cw"].wait()
    loads["pk"].wait()
    spec = mm(half_way, f["cw"], 1, 1)
    lams = f["pk"][16:24, :]
    p2 = f["pk"][0:8, :]
    p1 = f["pk"][24:32, :n]
    m8 = f["pk"][24:32, n:]
    columns = jnp.concatenate([lams[0:2, :n], p1[0:6]], axis=0).T
    weight = 1.0 / (columns[:, 1:2] + lams[0:1] + g)
    sol = weight * spec
    spec_v[...] = spec
    weight_v[...] = weight
    by_row = jnp.sum((sol * columns[:, 2:3]).reshape(n // 8, 8, w), axis=0)
    by_col = fold_lanes(sol * p2[0:1], min(w, 128))
    sign_row = 1.0 - 2.0 * (lax.broadcasted_iota(jnp.int32, (8, 1), 0) % 2).astype(jnp.float32)
    zf = jnp.sum(by_row, axis=0, keepdims=True)
    zl = jnp.sum(by_row * sign_row, axis=0, keepdims=True)
    signs_lane = 1.0 - 2.0 * (lax.broadcasted_iota(jnp.int32, (8, by_col.shape[1]), 1) % 2).astype(jnp.float32)
    odd_row = lax.broadcasted_iota(jnp.int32, (8, by_col.shape[1]), 0) % 2 == 1
    zb = mm(jnp.where(odd_row, signs_lane, 1.0), by_col, 1, 1)
    cut = lambda x: [x[:, i * M : (i + 1) * M] for i in range(x.shape[1] // M)]
    out1[...] = jnp.concatenate(cut(zf) + cut(zl) + cut(zb[0:1]) + cut(zb[1:2]), axis=0)
    pl.semaphore_wait(barrier, half + C - 1 + far_most)
    row_start(out1, buf1, s1, v1, o1, far1)

    for name in rest:
        loads[name].wait()
    dev = f["dev"][...]
    base, far = chain(lams[0:1] + g, n)
    inv_v[...] = 1.0 / (base + far * f["s2"][...][:, 0:1])
    own_energy = fold_lanes(jnp.sum(spec_v[...] * spec_v[...] * weight_v[...], axis=0, keepdims=True), M)
    store3(w3, weight_v[...])
    store3(c3, f["cn"][...])
    store3(t3, f["tab"][...])
    row_finish(out1, buf1, s1, v1, o1, far1)
    wide_rows = lambda first, count: jnp.concatenate(
        [buf1[:, first + k, :] for k in range(count)], axis=1
    )
    last, head = wide_rows(4, 4), wide_rows(0, 4)
    jump = last - jnp.concatenate([head[1:], head[:1]], axis=0)
    yl = jnp.dot(f["qe"][:, : 6 * R].astype(jnp.bfloat16), tall6(jump), preferred_element_type=jnp.float32)
    mixed = jnp.dot(dev[0:8, : 6 * R].astype(jnp.bfloat16), tall6(wide_rows(8, 4)), preferred_element_type=jnp.float32)
    yl_v[...] = yl
    tl = yl * inv_v[...]
    energy_r = fold_lanes(jnp.sum(yl * tl, axis=0, keepdims=True), M)
    q8 = jnp.dot(dev[8:16, : 6 * R].astype(jnp.bfloat16), tall6(tl), preferred_element_type=jnp.float32)
    q8 = jnp.concatenate([q8[0:4], q8[0:4]], axis=0) * f["pk"][8:16, :]
    v8 = mm6(q8, w3, 1, 1) * m8
    z4 = jnp.concatenate(
        [
            mixed[0:1, :n] + v8[0:1] + v8[2:3],
            mixed[0:1, n:] + v8[4:5] + v8[6:7],
            mixed[1:2, :n] + v8[1:2] + v8[3:4],
            mixed[1:2, n:] + v8[5:6] + v8[7:8],
            jnp.zeros((4, n), jnp.float32),
        ],
        axis=0,
    )
    zp = mm6(z4, c3)
    re, im = zp[0:2], zp[2:4]
    rot = dev[24:32, :n]
    a1 = re * rot[0:1] + im * rot[1:2]
    b1 = re * rot[2:3] + im * rot[3:4]
    a2 = re * rot[4:5] + im * rot[5:6]
    b2 = re * rot[6:7] + im * rot[7:8]
    yy = mm6(jnp.concatenate([a1, a2, b1, b2], axis=0), t3)
    y4 = yy[0:4, :M] - yy[4:8, M:]
    out2[...] = jnp.concatenate([y4, own_energy - energy_r * (1.0 / R)], axis=0)

    @pl.loop(1, C)
    def _(i):
        peer = lax.rem(col + i, C)
        col_copy(col, peer).start()

    buf2[col] = out2[...]

    base, far = chain(dev[34:35, : 2 * M] + g, w)
    norm = dev[35:36, : 2 * M]
    inv_c = norm / (base + far * f["s2"][...][:C, 1:2])
    cwh[...], cwl[...] = split(f["cw"][...])
    cth[...], ctl[...] = split(f["cn"][...].T)

    wait_tiles(buf2, C - 1, v2)

    pick2 = lambda a, b: jnp.concatenate([buf2[:, a, :], buf2[:, b, :]], axis=1)
    last, head = pick2(1, 3), pick2(0, 2)
    jump = last - jnp.concatenate([head[1:], head[:1]], axis=0)
    y = jnp.dot(f["qc"][:, : 6 * C].astype(jnp.bfloat16), tall6(jump), preferred_element_type=jnp.float32)
    tl = y * inv_c
    energy = jnp.sum(buf2[:, 4, :], axis=0, keepdims=True) - fold_lanes(jnp.sum(y * tl, axis=0, keepdims=True), M)
    q2 = jnp.dot(f["devc"][...][:, : 6 * C].astype(jnp.bfloat16), tall6(tl), preferred_element_type=jnp.float32)
    q4 = jnp.concatenate([q2[0:2, :M], q2[0:2, M:], jnp.zeros((4, M), jnp.float32)], axis=0)
    u = mm6(q4, [ref[:M, :M] for ref in t3], 1, 1)
    v = mm6(q4, [ref[:M, M:] for ref in t3], 1, 1)
    rot = rot[:, :M]
    re = u[0:2] * rot[0:1] - v[0:2] * rot[2:3] + u[2:4] * rot[4:5] - v[2:4] * rot[6:7]
    im = u[0:2] * rot[1:2] - v[0:2] * rot[3:4] + u[2:4] * rot[5:6] - v[2:4] * rot[7:8]
    out3[...] = jnp.concatenate([re, im, energy], axis=0)
    row_start(out3, buf3, s3, v3, o3, far3)
    wait_tiles(buf1, R - 1, s1)
    wait_tiles(buf2, C - 1, s2)
    row_finish(out3, buf3, s3, v3, o3, far3)

    pick3 = lambda a, b: jnp.concatenate([buf3[:, a, :], buf3[:, b, :]], axis=1)
    parts = tall6(jnp.concatenate([pick3(0, 1), pick3(2, 3)], axis=0))
    own = jnp.concatenate([dev[16:24, : 8 * R], dev[40:48, : 4 * R]], axis=1)
    lhs = jnp.concatenate([f["x3"][...], own], axis=0).astype(jnp.bfloat16)
    xx = jnp.dot(lhs, parts, preferred_element_type=jnp.float32)
    inner = jnp.sum(jnp.sum(buf3[:, 4, :], axis=0, keepdims=True), axis=1, keepdims=True)
    xx = jnp.concatenate([xx[:, :M], xx[:, M:]], axis=0)
    xc = mm6(xx, [ref[:, :M] for ref in c3], 1, 1)
    half_src = lambda at: xc[at : at + R] * m8[0:1] + xc[at + R : at + 2 * R] * m8[2:3]
    right_at = 2 * R + 8
    moved = mm6(jnp.concatenate([half_src(0), half_src(right_at)], axis=0), w3)
    y_all = yl_v[...] + moved[:R] * p2[0:1] + moved[R:] * p2[1:2]
    row_flux = jnp.dot(dev[32:40, : 6 * R].astype(jnp.bfloat16), tall6(y_all * inv_v[...]), preferred_element_type=jnp.float32)
    side = lambda at: xc[at : at + 1] * lams[2:3, :n] + xc[at + 1 : at + 2] * lams[3:4, :n]
    left = jnp.concatenate([p1[0:2], side(2 * R), side(right_at + 2 * R), p1[4:8]], axis=0)
    right = jnp.concatenate([row_flux[0:2], p2[0:2], p2[4:8]], axis=0)
    high, mid, low = split3(left)
    tall = jnp.concatenate([high, mid, low, high, mid, high], axis=0)
    low_rank = jnp.dot(tall.T.astype(jnp.bfloat16), tall6(right), preferred_element_type=jnp.float32)
    sol = weight_v[...] * (spec_v[...] + low_rank)
    wide = mm3(split(sol), (cwh, cwl))
    precond = mm3((cth, ctl), split(wide))
    next_ref[...] = precond
    inner_ref[...] = jnp.broadcast_to(inner, inner_ref.shape)
    wait_tiles(buf3, R - 1, s3)


def finish(scalar_ref, inner_ref, precond_ref, direction_ref, next_ref, ratio_ref):
    ratio = inner_ref[0:1, 0:1] / scalar_ref[1:2, 0:1]
    next_ref[...] = precond_ref[...] + ratio * direction_ref[...]
    ratio_ref[0] = jnp.sum(ratio)


def solution(mesh):
    R, C = mesh.shape["row"], mesh.shape["col"]

    def body(residual, direction, ground_shift, previous):
        n, w = residual.shape
        M = n // 2
        tables = make_tables(n, w, R, C)
        names = tuple(tables)
        shapes = [v.shape[1:] if k in ("dev", "devc") else v.shape for k, v in tables.items()]
        smem = pl.BlockSpec(memory_space=pltpu.SMEM)
        hbm = pl.BlockSpec(memory_space=pltpu.HBM)
        f32, bf16 = jnp.float32, jnp.bfloat16
        vm = lambda *shape: pltpu.VMEM(shape, f32)
        vb = lambda *shape: pltpu.VMEM(shape, bf16)
        dma = pltpu.SemaphoreType.DMA
        vmem = pl.BlockSpec(memory_space=pltpu.VMEM)
        held = lambda x: pltpu.with_memory_space_constraint(x, pltpu.HBM)
        lane = lax.broadcasted_iota(jnp.int32, (8, 128), 0)
        scalars = jnp.where(lane == 0, ground_shift, previous)
        precond, inner = pl.pallas_call(
            functools.partial(kernel, names, R, C),
            out_shape=(jax.ShapeDtypeStruct((n, w), f32), jax.ShapeDtypeStruct((8, 128), f32)),
            in_specs=[vmem] + [hbm] * (1 + len(names)),
            out_specs=(vmem, vmem),
            scratch_shapes=[pltpu.VMEM(s, f32) for s in shapes]
            + [vm(n, w), vm(12, M), vm(5, M), vm(5, M)]
            + [vm(R, 12, M), vm(C, 5, M), vm(R, 5, M)]
            + [vm(n, w), vm(n, w), vm(R, w), vm(R, w), vb(w, w), vb(w, w), vb(n, n), vb(n, n)]
            + [vb(n, w)] * 3 + [vb(n, n)] * 3 + [vb(n, n)] * 3
            + [dma((len(names) + 1,)), dma, dma((R // 2,)), dma, dma, dma, dma, dma((R // 2,)), dma],
            compiler_params=pltpu.CompilerParams(
                collective_id=0, has_side_effects=True, vmem_limit_bytes=24 * 2**20
            ),
        )(scalars, held(residual), *[held(jnp.asarray(v)) for v in tables.values()])
        return pl.pallas_call(
            finish,
            out_shape=(jax.ShapeDtypeStruct((n, w), f32), jax.ShapeDtypeStruct((1,), f32)),
            in_specs=[vmem] * 4,
            out_specs=(vmem, smem),
            compiler_params=pltpu.CompilerParams(vmem_limit_bytes=8 * 2**20),
        )(scalars, inner, precond, direction)

    return jax.shard_map(
        body,
        mesh=mesh,
        in_specs=(P("row", "col"), P("row", "col"), P(), P()),
        out_specs=(P("row", "col"), P()),
        check_vma=False,
    )
```

```python
import functools
import jax
import jax.numpy as jnp
import numpy as np
from jax import lax
from jax.experimental import pallas as pl
from jax.experimental.pallas import tpu as pltpu
from jax.sharding import PartitionSpec as P

HI = lax.Precision.HIGHEST
FAR1 = 0
FAR3 = 15


def mm(a, b, ca=1, cb=0):
    return lax.dot_general(
        a[...], b[...], (((ca,), (cb,)), ((), ())), precision=HI, preferred_element_type=jnp.float32
    )


def dct_table(n):
    k = np.arange(n)[:, None]
    p = np.arange(n)[None, :]
    table = np.sqrt(2.0 / n) * np.cos(np.pi * (k * (2 * p + 1) % (4 * n)) / (2 * n))
    table[0] = np.sqrt(1.0 / n)
    return table


def edge_sines(blocks):
    e = np.arange(1, blocks)
    q = np.zeros((blocks, blocks))
    q[: blocks - 1, : blocks - 1] = np.sqrt(2.0 / blocks) * np.sin(
        np.pi * (np.outer(e, e) % (2 * blocks)) / blocks
    )
    return q


def stack6(a):
    cut = lambda x: x.astype(np.float32).astype(jnp.bfloat16).astype(np.float64)
    high = cut(a)
    mid = cut(a - high)
    low = cut(a - high - mid)
    return np.concatenate([high, mid, low, high, mid, high], axis=-1)


def make_tables(n, w, R, C):
    assert w == 2 * n and R % 2 == 0 and C <= R
    M = n // 2
    f = {}
    cn, cw = dct_table(n), dct_table(w)
    even = np.where(np.arange(n) % 2 == 0, 1.0, 0.0)
    phi, sgn = cn[:, 0], 2 * even - 1
    phj, sgj = cw[:, 0], np.where(np.arange(w) % 2 == 0, 1.0, -1.0)
    f["cw"], f["cn"] = cw, cn
    pk = np.zeros((32, w))
    pk[0], pk[1] = phj, sgj * phj
    pk[8:12], pk[12:16] = phj, sgj * phj
    pk[16] = 4 * np.sin(np.pi * np.arange(w) / (2 * w)) ** 2
    pk[17, :n] = 4 * np.sin(np.pi * np.arange(n) / (2 * n)) ** 2
    pk[18, :n], pk[19, :n] = even, 1 - even
    pk[24, :n], pk[25, :n] = phi, sgn * phi
    for i in range(8):
        pk[24 + i, n:] = phi * (even if i in (0, 1, 4, 5) else 1 - even)
    f["pk"] = pk
    s2 = np.zeros((R, 128))
    s2[:, 0] = np.sin(np.pi * np.arange(1, R + 1) / (2 * R)) ** 2
    s2[:C, 1] = np.sin(np.pi * np.arange(1, C + 1) / (2 * C)) ** 2
    f["s2"] = s2

    t = np.arange(R)[:, None]
    d = np.arange(R)[None, :]
    ang = np.pi * (t * d % (2 * R)) / R
    mix_c, mix_s = np.cos(ang), np.sin(ang)
    mix_s[0] = np.where(np.arange(R) % 2 == 0, 1.0, -1.0)
    q_r, q_c = edge_sines(R), edge_sines(C)
    shift_r, shift_c = np.zeros((R, R)), np.zeros((C, C))
    shift_r[1:], shift_c[1:] = q_r[:-1], q_c[:-1]

    f["qe"] = np.zeros((R, max(256, 6 * R)))
    f["qe"][:, : 6 * R] = stack6(q_r.T)
    f["qc"] = np.zeros((C, max(128, 6 * C)))
    f["qc"][:, : 6 * C] = stack6(q_c.T)
    alt = np.where(np.arange(R) % 2 == 0, 1.0, -1.0)[:, None]
    fold = lambda mix, sign: mix + sign * alt * mix[:, ::-1]
    nxt = lambda m: np.concatenate([m[:, 1:], np.zeros((R, 1))], axis=1)
    x3 = np.zeros((2, R, 2 * R))
    for part, mix in ((0, mix_c), (R, mix_s)):
        ev, od = fold(mix, 1.0), fold(mix, -1.0)
        x3[0, :, part : part + R] = q_r.T @ (ev - nxt(ev)).T
        x3[1, :, part : part + R] = -q_r.T @ (od + nxt(od)).T
    f["x3"] = stack6(x3.reshape(2 * R, 2 * R))

    p = np.arange(n)[:, None]
    m = np.arange(M)[None, :]
    a_ang = np.pi * (m * (2 * p + 1) % (2 * n)) / n
    f["tab"] = np.concatenate([np.cos(a_ang), np.sin(a_ang)], axis=1)

    lanes = max(8 * R, n, 2 * M, 256)
    dev = np.zeros((R, 48, lanes))
    pos = 2 * np.arange(n) + 1
    N = n * R
    for r in range(R):
        nz = float(r > 0)
        dev[r, 0, : 6 * R] = stack6(mix_c[r])
        dev[r, 1, : 6 * R] = stack6(mix_s[r])
        for part, mix in ((0, mix_c), (1, mix_s)):
            top = mix[r] @ shift_r
            bot = -(mix[r] @ q_r)
            dev[r, 8 + part, : 6 * R] = stack6(top + bot)
            dev[r, 10 + part, : 6 * R] = stack6(top - bot)
        dev[r, 32, : 6 * R] = stack6(shift_r[r])
        dev[r, 33, : 6 * R] = stack6(-q_r[r])
        for base, sign in ((0, 1.0), (1, -1.0)):
            both = np.concatenate([fold(mix_c, sign)[:, r], fold(mix_s, sign)[:, r]])
            first, second = np.split(stack6(both), [8 * R])
            dev[r, 16 + base, : 8 * R] = first
            dev[r, 40 + base, : 4 * R] = second
        tau = (r, 2 * R - r if r > 0 else R)
        ca, sa = [], []
        for x in tau:
            b = np.pi * (x * pos % (4 * N)) / (2 * N)
            ca.append(np.cos(b))
            sa.append(np.sin(b))
        rot = [ca[0], -nz * sa[0], sa[0], nz * ca[0]]
        if r > 0:
            rot += [ca[1], sa[1], sa[1], -ca[1]]
        else:
            rot += [0 * pos, ca[1], 0 * pos, sa[1]]
        for i, v in enumerate(rot):
            dev[r, 24 + i, :n] = v
        k = np.concatenate([2 * R * np.arange(M) + x for x in tau])
        dev[r, 34, : 2 * M] = 4 * np.sin(np.pi * k / (2 * N)) ** 2
        dev[r, 35, : 2 * M] = np.where(k == 0, 1.0 / N, 2.0 / N)
    f["dev"] = dev
    devc = np.zeros((C, 8, 128))
    for c in range(C):
        devc[c, 0, : 6 * C] = stack6(shift_c[c])
        devc[c, 1, : 6 * C] = stack6(-q_c[c])
    f["devc"] = devc
    return {key: v.astype(np.float32) for key, v in f.items()}


def chain(mu, n):
    s = 0.5 * jnp.sqrt(mu)
    ch = jnp.sqrt(1.0 + s * s)
    x = s + s * s / (1.0 + ch)
    z = x / (2.0 + x)
    z2 = z * z
    acc = jnp.full_like(z, 1.0 / 19.0)
    for k in (17, 15, 13, 11, 9, 7, 5, 3, 1):
        acc = acc * z2 + 1.0 / k
    theta = 4.0 * z * acc
    decay = jnp.exp(-n * theta)
    shorter = jnp.exp(-(n - 1) * theta)
    diff = (ch - s) * (1.0 - shorter) / (2.0 * s * (1.0 + decay))
    far = ch * decay / (s * (1.0 - decay * decay))
    return 1.0 + 2.0 * diff, 4.0 * far


def split(x):
    high = x.astype(jnp.bfloat16)
    return high, (x - high.astype(jnp.float32)).astype(jnp.bfloat16)


def mm3(a, b):
    dot = lambda x, y: jnp.dot(x[...], y[...], preferred_element_type=jnp.float32)
    return dot(a[0], b[0]) + (dot(a[0], b[1]) + dot(a[1], b[0]))


def split3(x):
    high = x.astype(jnp.bfloat16).astype(jnp.float32)
    rest = x - high
    mid = rest.astype(jnp.bfloat16).astype(jnp.float32)
    return high, mid, rest - mid


def store3(refs, x):
    for ref, part in zip(refs, split3(x)):
        ref[...] = part.astype(jnp.bfloat16)


def mm6(a, b, ca=1, cb=0):
    rows = a.shape[0]
    a3 = jnp.concatenate(split3(a), axis=0).astype(jnp.bfloat16)
    dot = lambda x, y: lax.dot_general(
        x, y[...], (((ca,), (cb,)), ((), ())), preferred_element_type=jnp.float32
    )
    p0, p1, p2 = dot(a3, b[0]), dot(a3[: 2 * rows], b[1]), dot(a3[: 2 * rows], b[2])
    low = p0[2 * rows :] + p1[rows:] + p2[:rows]
    return p0[:rows] + (p0[rows : 2 * rows] + p1[:rows] + low)


def tall6(b):
    high, mid, low = split3(b)
    return jnp.concatenate([high, high, high, mid, mid, low], axis=0).astype(jnp.bfloat16)


def fold_lanes(x, width):
    out = x[:, :width]
    for i in range(1, x.shape[1] // width):
        out = out + x[:, i * width : (i + 1) * width]
    return out


MESH_ID = pl.DeviceIdType.MESH


def kernel(names, R, C, *refs):
    count = len(names)
    scalar_ref, residual_ref = refs[:2]
    table_hbm = refs[2 : 2 + count]
    next_ref, inner_ref = refs[2 + count : 4 + count]
    refs = refs[4 + count :]
    table_v, refs = refs[:count], refs[count:]
    (r_v, out1, out2, out3, buf1, buf2, buf3), refs = refs[:7], refs[7:]
    (spec_v, weight_v, yl_v, inv_v, cwh, cwl, cth, ctl), refs = refs[:8], refs[8:]
    w3, c3, t3, refs = refs[:3], refs[3:6], refs[6:9], refs[9:]
    load_sem, s1, v1, o1, s2, v2, s3, v3, o3 = refs
    row, col = lax.axis_index("row"), lax.axis_index("col")
    half = R // 2
    partner = row + 1 - 2 * lax.rem(row, 2)
    n, w = r_v.shape
    M = n // 2
    far1, far3 = min(FAR1, half - 1), min(FAR3, half - 1)
    far_most = max(far1, far3)

    def chip_step(j):
        return half // 2 + lax.div(j + 1, 2) * (1 - 2 * lax.rem(j, 2))


    loads = {}
    for i, name in enumerate(names):
        src = table_hbm[i]
        if name == "dev":
            src = src.at[row]
        elif name == "devc":
            src = src.at[col]
        loads[name] = pltpu.make_async_copy(src, table_v[i], load_sem.at[i])
    loads["residual"] = pltpu.make_async_copy(residual_ref, r_v, load_sem.at[count])
    first = ("cn", "residual", "cw", "pk")
    rest = tuple(x for x in names if x not in first)
    for name in first:
        loads[name].start()

    barrier = pltpu.get_barrier_semaphore()

    @pl.loop(1, half)
    def _(i):
        peer = lax.rem(row + 2 * i, R)
        pl.semaphore_signal(barrier, inc=1, device_id=(peer, col), device_id_type=MESH_ID)

    @pl.loop(1, C)
    def _(i):
        peer = lax.rem(col + i, C)
        pl.semaphore_signal(barrier, inc=1, device_id=(row, peer), device_id_type=MESH_ID)

    @pl.loop(0, far_most)
    def _(j):
        peer = lax.rem(partner + 2 * chip_step(j), R)
        pl.semaphore_signal(barrier, inc=1, device_id=(peer, col), device_id_type=MESH_ID)

    pl.semaphore_signal(barrier, inc=1, device_id=(partner, col), device_id_type=MESH_ID)

    for name in rest:
        loads[name].start()
    f = dict(zip(names, table_v))
    g = scalar_ref[0:1, 0:1]

    def tile(buf, slot):
        return buf.at[slot]

    def row_copy(src, buf, slot, send, recv, peer):
        return pltpu.make_async_remote_copy(
            src_ref=src,
            dst_ref=tile(buf, slot),
            send_sem=send,
            recv_sem=recv,
            device_id=(peer, col),
            device_id_type=MESH_ID,
        )

    def wait_tiles(buf, tiles, sem):
        part = buf.at[pl.ds(0, tiles)]
        pltpu.make_async_copy(part, part, sem).wait()

    def row_start(out, buf, send, same, other, far_both):
        @pl.loop(0, far_both)
        def _(j):
            i = chip_step(j)
            chip = lax.div(row, 2)
            row_copy(out, buf, row, send, same.at[chip], lax.rem(row + 2 * i, R)).start()
            row_copy(out, buf, row, send, other, lax.rem(partner + 2 * i, R)).start()

        @pl.loop(far_both, half - 1)
        def _(j):
            i = chip_step(j)
            chip = lax.div(row, 2)
            row_copy(out, buf, row, send, same.at[chip], lax.rem(row + 2 * i, R)).start()

        row_copy(out, buf, row, send, other, partner).start()
        buf[row] = out[...]

    def row_finish(out, buf, send, same, other, far_both):
        @pl.loop(0, half - 1 - far_both)
        def _(j):
            slot = lax.rem(row + 2 * chip_step(half - 2 - j), R)
            row_copy(out, buf, slot, send, same.at[lax.div(slot, 2)], partner).wait_recv()
            row_copy(tile(buf, slot), buf, slot, send, other, partner).start()

        @pl.loop(0, far_both)
        def _(j):
            slot = lax.rem(row + 2 * chip_step(j), R)
            row_copy(out, buf, slot, send, same.at[lax.div(slot, 2)], partner).wait_recv()

        wait_tiles(buf, half, other)

    def col_copy(slot, peer):
        return pltpu.make_async_remote_copy(
            src_ref=out2,
            dst_ref=tile(buf2, slot),
            send_sem=s2,
            recv_sem=v2,
            device_id=(row, peer),
            device_id_type=MESH_ID,
        )

    loads["cn"].wait()
    loads["residual"].wait()
    half_way = mm(f["cn"], r_v)
    loads["cw"].wait()
    loads["pk"].wait()
    spec = mm(half_way, f["cw"], 1, 1)
    lams = f["pk"][16:24, :]
    p2 = f["pk"][0:8, :]
    p1 = f["pk"][24:32, :n]
    m8 = f["pk"][24:32, n:]
    columns = jnp.concatenate([lams[0:2, :n], p1[0:6]], axis=0).T
    weight = 1.0 / (columns[:, 1:2] + lams[0:1] + g)
    sol = weight * spec
    spec_v[...] = spec
    weight_v[...] = weight
    by_row = jnp.sum((sol * columns[:, 2:3]).reshape(n // 8, 8, w), axis=0)
    by_col = fold_lanes(sol * p2[0:1], min(w, 128))
    sign_row = 1.0 - 2.0 * (lax.broadcasted_iota(jnp.int32, (8, 1), 0) % 2).astype(jnp.float32)
    zf = jnp.sum(by_row, axis=0, keepdims=True)
    zl = jnp.sum(by_row * sign_row, axis=0, keepdims=True)
    signs_lane = 1.0 - 2.0 * (lax.broadcasted_iota(jnp.int32, (8, by_col.shape[1]), 1) % 2).astype(jnp.float32)
    odd_row = lax.broadcasted_iota(jnp.int32, (8, by_col.shape[1]), 0) % 2 == 1
    pattern = jnp.where(odd_row, signs_lane, 1.0)
    zb = lax.dot_general(
        jnp.concatenate([pattern] * 3, axis=1).astype(jnp.bfloat16),
        jnp.concatenate(split3(by_col), axis=1).astype(jnp.bfloat16),
        (((1,), (1,)), ((), ())),
        preferred_element_type=jnp.float32,
    )
    cut = lambda x: [x[:, i * M : (i + 1) * M] for i in range(x.shape[1] // M)]
    out1[...] = jnp.concatenate(cut(zf) + cut(zl) + cut(zb[0:1]) + cut(zb[1:2]), axis=0)
    pl.semaphore_wait(barrier, half + C - 1 + far_most)
    row_start(out1, buf1, s1, v1, o1, far1)

    for name in rest:
        loads[name].wait()
    dev = f["dev"][...]
    base, far = chain(lams[0:1] + g, n)
    inv_v[...] = 1.0 / (base + far * f["s2"][...][:, 0:1])
    own_energy = fold_lanes(jnp.sum(spec_v[...] * spec_v[...] * weight_v[...], axis=0, keepdims=True), M)
    store3(w3, weight_v[...])
    store3(c3, f["cn"][...])
    store3(t3, f["tab"][...])
    row_finish(out1, buf1, s1, v1, o1, far1)
    wide_rows = lambda first, count: jnp.concatenate(
        [buf1[:, first + k, :] for k in range(count)], axis=1
    )
    last, head = wide_rows(4, 4), wide_rows(0, 4)
    jump = last - jnp.concatenate([head[1:], head[:1]], axis=0)
    yl = jnp.dot(f["qe"][:, : 6 * R].astype(jnp.bfloat16), tall6(jump), preferred_element_type=jnp.float32)
    mixed = jnp.dot(dev[0:8, : 6 * R].astype(jnp.bfloat16), tall6(wide_rows(8, 4)), preferred_element_type=jnp.float32)
    yl_v[...] = yl
    tl = yl * inv_v[...]
    energy_r = fold_lanes(jnp.sum(yl * tl, axis=0, keepdims=True), M)
    q8 = jnp.dot(dev[8:16, : 6 * R].astype(jnp.bfloat16), tall6(tl), preferred_element_type=jnp.float32)
    q8 = jnp.concatenate([q8[0:4], q8[0:4]], axis=0) * f["pk"][8:16, :]
    v8 = mm6(q8, w3, 1, 1) * m8
    z4 = jnp.concatenate(
        [
            mixed[0:1, :n] + v8[0:1] + v8[2:3],
            mixed[0:1, n:] + v8[4:5] + v8[6:7],
            mixed[1:2, :n] + v8[1:2] + v8[3:4],
            mixed[1:2, n:] + v8[5:6] + v8[7:8],
            jnp.zeros((4, n), jnp.float32),
        ],
        axis=0,
    )
    zp = mm6(z4, c3)
    re, im = zp[0:2], zp[2:4]
    rot = dev[24:32, :n]
    a1 = re * rot[0:1] + im * rot[1:2]
    b1 = re * rot[2:3] + im * rot[3:4]
    a2 = re * rot[4:5] + im * rot[5:6]
    b2 = re * rot[6:7] + im * rot[7:8]
    yy = mm6(jnp.concatenate([a1, a2, b1, b2], axis=0), t3)
    y4 = yy[0:4, :M] - yy[4:8, M:]
    out2[...] = jnp.concatenate([y4, own_energy - energy_r * (1.0 / R)], axis=0)

    @pl.loop(1, C)
    def _(i):
        peer = lax.rem(col + i, C)
        col_copy(col, peer).start()

    buf2[col] = out2[...]

    base, far = chain(dev[34:35, : 2 * M] + g, w)
    norm = dev[35:36, : 2 * M]
    inv_c = norm / (base + far * f["s2"][...][:C, 1:2])
    cwh[...], cwl[...] = split(f["cw"][...])
    cth[...], ctl[...] = split(f["cn"][...].T)

    wait_tiles(buf2, C - 1, v2)

    pick2 = lambda a, b: jnp.concatenate([buf2[:, a, :], buf2[:, b, :]], axis=1)
    last, head = pick2(1, 3), pick2(0, 2)
    jump = last - jnp.concatenate([head[1:], head[:1]], axis=0)
    y = jnp.dot(f["qc"][:, : 6 * C].astype(jnp.bfloat16), tall6(jump), preferred_element_type=jnp.float32)
    tl = y * inv_c
    energy = jnp.sum(buf2[:, 4, :], axis=0, keepdims=True) - fold_lanes(jnp.sum(y * tl, axis=0, keepdims=True), M)
    q2 = jnp.dot(f["devc"][...][:, : 6 * C].astype(jnp.bfloat16), tall6(tl), preferred_element_type=jnp.float32)
    q4 = jnp.concatenate([q2[0:2, :M], q2[0:2, M:], jnp.zeros((4, M), jnp.float32)], axis=0)
    u = mm6(q4, [ref[:M, :M] for ref in t3], 1, 1)
    v = mm6(q4, [ref[:M, M:] for ref in t3], 1, 1)
    rot = rot[:, :M]
    re = u[0:2] * rot[0:1] - v[0:2] * rot[2:3] + u[2:4] * rot[4:5] - v[2:4] * rot[6:7]
    im = u[0:2] * rot[1:2] - v[0:2] * rot[3:4] + u[2:4] * rot[5:6] - v[2:4] * rot[7:8]
    out3[...] = jnp.concatenate([re, im, energy], axis=0)
    row_start(out3, buf3, s3, v3, o3, far3)
    wait_tiles(buf1, R - 1, s1)
    wait_tiles(buf2, C - 1, s2)
    row_finish(out3, buf3, s3, v3, o3, far3)

    pick3 = lambda a, b: jnp.concatenate([buf3[:, a, :], buf3[:, b, :]], axis=1)
    parts = tall6(jnp.concatenate([pick3(0, 1), pick3(2, 3)], axis=0))
    own = jnp.concatenate([dev[16:24, : 8 * R], dev[40:48, : 4 * R]], axis=1)
    lhs = jnp.concatenate([f["x3"][...], own], axis=0).astype(jnp.bfloat16)
    xx = jnp.dot(lhs, parts, preferred_element_type=jnp.float32)
    inner = jnp.sum(jnp.sum(buf3[:, 4, :], axis=0, keepdims=True), axis=1, keepdims=True)
    xx = jnp.concatenate([xx[:, :M], xx[:, M:]], axis=0)
    xc = mm6(xx, [ref[:, :M] for ref in c3], 1, 1)
    half_src = lambda at: xc[at : at + R] * m8[0:1] + xc[at + R : at + 2 * R] * m8[2:3]
    right_at = 2 * R + 8
    moved = mm6(jnp.concatenate([half_src(0), half_src(right_at)], axis=0), w3)
    y_all = yl_v[...] + moved[:R] * p2[0:1] + moved[R:] * p2[1:2]
    row_flux = jnp.dot(dev[32:40, : 6 * R].astype(jnp.bfloat16), tall6(y_all * inv_v[...]), preferred_element_type=jnp.float32)
    side = lambda at: xc[at : at + 1] * lams[2:3, :n] + xc[at + 1 : at + 2] * lams[3:4, :n]
    left = jnp.concatenate([p1[0:2], side(2 * R), side(right_at + 2 * R), p1[4:8]], axis=0)
    right = jnp.concatenate([row_flux[0:2], p2[0:2], p2[4:8]], axis=0)
    high, mid, low = split3(left)
    tall = jnp.concatenate([high, mid, low, high, mid, high], axis=0)
    low_rank = jnp.dot(tall.T.astype(jnp.bfloat16), tall6(right), preferred_element_type=jnp.float32)
    sol = weight_v[...] * (spec_v[...] + low_rank)
    wide = mm3(split(sol), (cwh, cwl))
    precond = mm3((cth, ctl), split(wide))
    next_ref[...] = precond
    inner_ref[...] = jnp.broadcast_to(inner, inner_ref.shape)
    wait_tiles(buf3, R - 1, s3)


def finish(scalar_ref, inner_ref, precond_ref, direction_ref, next_ref, ratio_ref):
    ratio = inner_ref[0:1, 0:1] / scalar_ref[1:2, 0:1]
    next_ref[...] = precond_ref[...] + ratio * direction_ref[...]
    ratio_ref[0] = jnp.sum(ratio)


def solution(mesh):
    R, C = mesh.shape["row"], mesh.shape["col"]

    def body(residual, direction, ground_shift, previous):
        n, w = residual.shape
        M = n // 2
        tables = make_tables(n, w, R, C)
        names = tuple(tables)
        shapes = [v.shape[1:] if k in ("dev", "devc") else v.shape for k, v in tables.items()]
        smem = pl.BlockSpec(memory_space=pltpu.SMEM)
        hbm = pl.BlockSpec(memory_space=pltpu.HBM)
        f32, bf16 = jnp.float32, jnp.bfloat16
        vm = lambda *shape: pltpu.VMEM(shape, f32)
        vb = lambda *shape: pltpu.VMEM(shape, bf16)
        dma = pltpu.SemaphoreType.DMA
        vmem = pl.BlockSpec(memory_space=pltpu.VMEM)
        held = lambda x: pltpu.with_memory_space_constraint(x, pltpu.HBM)
        lane = lax.broadcasted_iota(jnp.int32, (8, 128), 0)
        scalars = jnp.where(lane == 0, ground_shift, previous)
        precond, inner = pl.pallas_call(
            functools.partial(kernel, names, R, C),
            out_shape=(jax.ShapeDtypeStruct((n, w), f32), jax.ShapeDtypeStruct((8, 128), f32)),
            in_specs=[vmem] + [hbm] * (1 + len(names)),
            out_specs=(vmem, vmem),
            scratch_shapes=[pltpu.VMEM(s, f32) for s in shapes]
            + [vm(n, w), vm(12, M), vm(5, M), vm(5, M)]
            + [vm(R, 12, M), vm(C, 5, M), vm(R, 5, M)]
            + [vm(n, w), vm(n, w), vm(R, w), vm(R, w), vb(w, w), vb(w, w), vb(n, n), vb(n, n)]
            + [vb(n, w)] * 3 + [vb(n, n)] * 3 + [vb(n, n)] * 3
            + [dma((len(names) + 1,)), dma, dma((R // 2,)), dma, dma, dma, dma, dma((R // 2,)), dma],
            compiler_params=pltpu.CompilerParams(
                collective_id=0, has_side_effects=True, vmem_limit_bytes=24 * 2**20
            ),
        )(scalars, held(residual), *[held(jnp.asarray(v)) for v in tables.values()])
        return pl.pallas_call(
            finish,
            out_shape=(jax.ShapeDtypeStruct((n, w), f32), jax.ShapeDtypeStruct((1,), f32)),
            in_specs=[vmem] * 4,
            out_specs=(vmem, smem),
            compiler_params=pltpu.CompilerParams(vmem_limit_bytes=8 * 2**20),
        )(scalars, inner, precond, direction)

    return jax.shard_map(
        body,
        mesh=mesh,
        in_specs=(P("row", "col"), P("row", "col"), P(), P()),
        out_specs=(P("row", "col"), P()),
        check_vma=False,
    )
```
